32 devices in a mesh: dp: 8 (over y, x, core), shard: 4 (over z).
Axes of the slice: x: 2, y: 2, z: 4, core: 2. Of those that a mesh axis runs over, the one named last changes fastest.
Arguments:
- tokens: bfloat16 [8, 1024, 2048], P('dp', 'shard'), may hold values from -6 to 6
- block_order: int32 [8, 8], P('dp'), may hold values from 0 to 7, as said below
- attn_gain: float32 [2048], P('shard'), may hold values from 0.1 to 1.9
- w_query: float32 [2048, 2048], P('shard'), may hold values from -0.125 to 0.125
- w_key: float32 [2048, 256], P('shard'), may hold values from -0.125 to 0.125
- w_value: float32 [2048, 256], P('shard'), may hold values from -0.125 to 0.125
- w_out: float32 [2048, 2048], P('shard'), may hold values from -0.75 to 0.75
- mlp_gain: float32 [2048], P('shard'), may hold values from 0.1 to 1.9
- w_gate: float32 [2048, 5632], P('shard'), may hold values from -0.125 to 0.125
- w_up: float32 [2048, 5632], P('shard'), may hold values from -0.125 to 0.125
- w_down: float32 [5632, 2048], P('shard'), may hold values from -0.078125 to 0.078125
- cotangent: bfloat16 [8, 1024, 2048], P('dp', 'shard'), may hold values from -6 to 6
Outputs:
- block_out: bfloat16 [8, 1024, 2048], P('dp', 'shard')
- tokens_grad: float32 [8, 1024, 2048], P('dp', 'shard')
- attn_gain_grad: float32 [2048], P('shard')
- w_query_grad: float32 [2048, 2048], P('shard')
- w_key_grad: float32 [2048, 256], P('shard')
- w_value_grad: float32 [2048, 256], P('shard')
- w_out_grad: float32 [2048, 2048], P('shard')
- mlp_gain_grad: float32 [2048], P('shard')
- w_gate_grad: float32 [2048, 5632], P('shard')
- w_up_grad: float32 [2048, 5632], P('shard')
- w_down_grad: float32 [5632, 2048], P('shard')
The draws below stay inside these ranges and needn't reach their ends.
Inputs may be any that keep to these rules, and one draw needn't show every extreme that they name: `block_order`: in each row every number of 0 to 7 appears once, and entries 2 j and 2 j + 1 of a row add up to 7.
All inputs are finite; a program needn't handle non-finite values.
Results may differ from the reference program's by a relative error of at most 0.023.
Values may be sent and summed in bfloat16 or wider, within the bound.
A program may use at most 448 MiB of HBM per device.

```python
import math
import jax
import jax.numpy as jnp
from jax import lax

D = 2048
FF = 5632
HEADS = 32
KV_HEADS = 4
HEAD_DIM = 64
LENGTH = 1024
SEQS = 8
BLOCKS = 8
BLOCK_ROWS = 128


def draw_block_order(key, part):
    half_count = BLOCKS // 2
    order_key, swap_key = jax.random.split(key)
    row_keys = jax.random.split(order_key, SEQS)

    def shuffle_row(row_key):
        return jax.random.permutation(row_key, half_count)
    shuffled = jax.vmap(shuffle_row)(row_keys).astype(jnp.int32)
    swapped = jax.random.randint(swap_key, (SEQS, half_count), 0, 2)
    leading = jnp.where(swapped == 1, BLOCKS - 1 - shuffled, shuffled)
    trailing = BLOCKS - 1 - leading
    return jnp.stack([leading, trailing], axis=-1).reshape(SEQS, BLOCKS).astype(jnp.int32)


def steps_of(rng, dims, cuts, smallest, high):
    gain = 1.0
    for axis_at, parts in cuts:
        heights = jax.random.uniform(jax.random.fold_in(jax.random.fold_in(rng, 6), axis_at), (parts,), jnp.float32, smallest / len(cuts), high / len(cuts))
        gain = gain * jnp.repeat(jnp.exp(heights), dims[axis_at] // parts).reshape((-1,) + (1,) * (len(dims) - 1 - axis_at))
    return gain


def centred(stream_key, extent, scale, bound, cuts=(), kind=jnp.bfloat16):
    entries = jax.random.normal(stream_key, extent, jnp.float32) * scale
    if len(cuts) > 0:
        entries = steps_of(stream_key, extent, cuts, -0.22, 0.18) * entries
    return jnp.clip(entries, min=-bound, max=bound).astype(kind)


def setup_inputs(seed: int = 0) -> dict:
    keys = jax.random.split(jax.random.key(seed), 13)
    return {
        "tokens": centred(keys[0], (SEQS, LENGTH, D), 1.0, 6.0, ((0, 8), (1, 4))),
        "block_order": draw_block_order(jax.random.fold_in(keys[12], 71), 0),
        "attn_gain": jnp.clip(1.0 + 0.18 * jax.random.normal(keys[2], (D,), jnp.float32), 0.1, 1.9),
        "w_query": centred(keys[3], (D, HEADS * HEAD_DIM), D ** -0.5, 0.125, ((0, 4),), jnp.float32),
        "w_key": centred(keys[4], (D, KV_HEADS * HEAD_DIM), D ** -0.5, 0.125, ((0, 4),), jnp.float32),
        "w_value": centred(keys[5], (D, KV_HEADS * HEAD_DIM), D ** -0.5, 0.125, ((0, 4),), jnp.float32),
        "w_out": centred(keys[6], (HEADS * HEAD_DIM, D), HEAD_DIM ** -0.5, 0.75, ((0, 4),), jnp.float32),
        "mlp_gain": jnp.clip(1.0 + 0.18 * jax.random.normal(keys[7], (D,), jnp.float32), 0.1, 1.9),
        "w_gate": centred(keys[8], (D, FF), D ** -0.5, 0.125, ((0, 4),), jnp.float32),
        "w_up": centred(keys[9], (D, FF), D ** -0.5, 0.125, ((0, 4),), jnp.float32),
        "w_down": centred(keys[10], (FF, D), FF ** -0.5, 0.078125, ((0, 4),), jnp.float32),
        "cotangent": centred(keys[11], (SEQS, LENGTH, D), 1.0, 6.0, ((0, 8), (1, 4))),
    }


EPSILON = 1e-05
ROPE_BASE = 10000.0
MASKED = -1e+30
HIGHEST = lax.Precision.HIGHEST

@jax.custom_vjp
def low(v):
    return lax.optimization_barrier(v.astype(jnp.bfloat16)).astype(jnp.float32)

@jax.custom_vjp
def low_back(v):
    return v

def low_keep(v):
    return (low(v), None)

def low_pass(kept, grad):
    return (grad,)

def back_keep(v):
    return (v, None)

def back_low(kept, grad):
    return (low(grad),)
low.defvjp(low_keep, low_pass)
low_back.defvjp(back_keep, back_low)

def matmul(left_side, right_side):
    return jnp.dot(left_side, right_side, precision=HIGHEST, preferred_element_type=jnp.float32)

def positions_of(order_row):
    places = jnp.arange(LENGTH, dtype=jnp.int32)
    return (order_row[places // BLOCK_ROWS] * BLOCK_ROWS + places % BLOCK_ROWS).astype(jnp.int32)

def rope_tables(positions):
    frequency = ROPE_BASE ** (-(jnp.arange(HEAD_DIM // 2, dtype=jnp.float32) * 2.0) / HEAD_DIM)
    angles = positions.astype(jnp.float32)[:, None] * frequency[None, :]
    return (jnp.cos(angles)[:, None, :], jnp.sin(angles)[:, None, :])

def rotate(values, cosine, sine_table):
    half_dim = values.shape[-1] // 2
    front_half = values[..., :half_dim]
    back_half = values[..., half_dim:]
    return jnp.concatenate([front_half * cosine - back_half * sine_table, back_half * cosine + front_half * sine_table], axis=-1)

def normalize(values, gain_vector):
    row_scale = lax.rsqrt(lax.optimization_barrier(jnp.mean(values * values, axis=-1, keepdims=True)) + EPSILON)
    return values * row_scale * gain_vector

def attend(queries, key_rot, values, positions):
    length = queries.shape[0]
    block_rows = min(512, length)
    blocks_count = length // block_rows

    def one_block(block_item):
        query_block, query_place = block_item
        scores = jnp.einsum('qhgd,khd->hgqk', query_block, key_rot, precision=HIGHEST) * HEAD_DIM ** (-0.5)
        scores = low_back(scores)
        visible = query_place[:, None] >= positions[None, :]
        scores = jnp.where(visible[None, None], scores, MASKED)
        row_top = lax.optimization_barrier(jnp.max(scores, axis=-1, keepdims=True))
        raw_weights = jnp.exp(scores - row_top)
        probability = low(raw_weights / lax.optimization_barrier(jnp.sum(raw_weights, axis=-1, keepdims=True)))
        return jnp.einsum('hgqk,khd->qhgd', probability, values, precision=HIGHEST)
    shaped = queries.reshape((blocks_count, block_rows) + queries.shape[1:])
    outputs = lax.map(jax.checkpoint(one_block), (shaped, positions.reshape(blocks_count, block_rows)))
    return outputs.reshape(queries.shape)

def layer(inputs, positions, attn_gain, w_query, w_key, w_value, w_out, mlp_gain, w_gate, w_up, w_down):
    length = inputs.shape[0]
    group_size = HEADS // KV_HEADS
    cosine, sine_table = rope_tables(positions)
    normed = low(normalize(inputs, low(attn_gain)))
    query_lin = low_back(matmul(normed, low(w_query))).reshape(length, HEADS, HEAD_DIM)
    key_lin = low_back(matmul(normed, low(w_key))).reshape(length, KV_HEADS, HEAD_DIM)
    value_lin = low_back(matmul(normed, low(w_value)))
    queries = low(rotate(query_lin, cosine, sine_table)).reshape(length, KV_HEADS, group_size, HEAD_DIM)
    key_rot = low(rotate(key_lin, cosine, sine_table))
    values = low(value_lin).reshape(length, KV_HEADS, HEAD_DIM)
    attended = attend(queries, key_rot, values, positions).reshape(length, HEADS * HEAD_DIM)
    attended = low(low_back(attended))
    branch = low_back(matmul(attended, low(w_out)))
    middle = inputs + branch
    normed_two = low(normalize(middle, low(mlp_gain)))
    gate_value = low_back(matmul(normed_two, low(w_gate)))
    up_value = low_back(matmul(normed_two, low(w_up)))
    hidden = low(jax.nn.silu(gate_value) * up_value)
    return middle + matmul(hidden, low(w_down))

def reference(tokens, block_order, attn_gain, w_query, w_key, w_value, w_out, mlp_gain, w_gate, w_up, w_down, cotangent):
    weights = (attn_gain, w_query, w_key, w_value, w_out, mlp_gain, w_gate, w_up, w_down)
    group_count = math.gcd(SEQS, max(1, 4096 // LENGTH))
    steps_count = SEQS // group_count
    inputs = tokens.astype(jnp.float32).reshape(steps_count, group_count, LENGTH, D)
    tangents = cotangent.astype(jnp.float32).reshape(steps_count, group_count, LENGTH, D)
    orders = block_order.reshape(steps_count, group_count, BLOCKS)

    def advance(totals, scan_item):
        input_group, tangent_group, order_group = scan_item
        places = jax.vmap(positions_of)(order_group)

        def forward(input_values, *params):

            def per_sequence(row_inputs, row_places):
                return layer(row_inputs, row_places, *params)
            return jax.vmap(per_sequence)(input_values, places)
        result, pullback = jax.vjp(forward, input_group, *weights)
        gradients = pullback(tangent_group)
        totals = tuple((running + gradient for running, gradient in zip(totals, gradients[1:])))
        return (totals, (result.astype(jnp.bfloat16), gradients[0]))
    initial = tuple((jnp.zeros_like(weight) for weight in weights))
    totals, (results, input_grads) = lax.scan(advance, initial, (inputs, tangents, orders))
    return (results.reshape(SEQS, LENGTH, D), input_grads.reshape(SEQS, LENGTH, D), totals[0], totals[1], totals[2], totals[3], totals[4], totals[5], totals[6], totals[7], totals[8])
```

```python
import jax
import jax.numpy as jnp
from jax import lax
from jax.sharding import PartitionSpec as P

HEAD_DIM = 64
EPSILON = 1e-05
ROPE_BASE = 10000.0
MASKED = -1e30
LOW = jnp.bfloat16
FULL = jnp.float32


def contract(left, right, left_dim, right_dim):
    return lax.dot_general(
        left, right, (((left_dim,), (right_dim,)), ((), ())), preferred_element_type=FULL
    )


def shift(value, amount):
    count = lax.axis_size("shard")
    pairs = [(i, (i + amount) % count) for i in range(count)]
    return lax.ppermute(value, "shard", pairs)


def plane_parts(value):
    count = lax.axis_size("shard")
    return [value] + [shift(value, k) for k in range(1, count)]


def assemble(parts, axis=0):
    count = lax.axis_size("shard")
    rank = lax.axis_index("shard")
    rows = parts[0].shape[axis]
    shape = list(parts[0].shape)
    shape[axis] = rows * count
    whole = jnp.zeros(shape, parts[0].dtype)
    for k, part in enumerate(parts):
        place = lax.rem(rank - k + count, count)
        whole = lax.dynamic_update_slice_in_dim(whole, part, place * rows, axis)
    return whole


def plane_scatter(value):
    count = lax.axis_size("shard")
    rank = lax.axis_index("shard")
    rows = value.shape[0] // count
    value = value.astype(LOW)
    total = None
    for k in range(count):
        target = lax.rem(rank + k, count)
        piece = lax.dynamic_slice_in_dim(value, target * rows, rows, 0)
        if k:
            piece = shift(piece, k)
        piece = piece.astype(FULL)
        total = piece if total is None else total + piece
    return total


def rope(values, cosine, sine):
    half = values.shape[-2] // 2
    front, back = values[..., :half, :], values[..., half:, :]
    return jnp.concatenate([front * cosine - back * sine, back * cosine + front * sine], axis=-2)


def places_of(table, plane, rows, span):
    blocks = rows // span
    count = table.shape[1] // blocks
    grouped = table.reshape(table.shape[0], count, blocks)
    picked = lax.dynamic_slice_in_dim(grouped, plane, 1, 1)[:, 0]
    within = jnp.arange(span, dtype=jnp.int32)
    return (picked[:, :, None] * span + within[None, None, :]).reshape(table.shape[0], rows)


def norm_back(upstream, normed, row_scale, gain):
    scaled = upstream * gain
    gain_grad = jnp.sum(upstream * normed, axis=0)
    mean = jnp.mean(scaled * normed, axis=-1, keepdims=True)
    return row_scale * (scaled - normed * mean), gain_grad


def on_device(
    tokens,
    block_order,
    attn_gain,
    w_query,
    w_key,
    w_value,
    w_out,
    mlp_gain,
    w_gate,
    w_up,
    w_down,
    cotangent,
):
    planes = lax.axis_size("shard")
    plane = lax.axis_index("shard")
    lanes = lax.axis_size("dp")
    lane = lax.axis_index("dp")
    rows = tokens.shape[1]
    width = tokens.shape[2]
    span = rows // 2
    seqs = lanes
    total_rows = seqs * rows
    own_width = width // planes
    heads = w_query.shape[1] // HEAD_DIM
    kv_heads = w_key.shape[1] // HEAD_DIM
    own_heads = heads // lanes
    head_cols = own_heads * HEAD_DIM
    kv_head = (lane * own_heads * kv_heads) // heads
    out_cols = w_out.shape[1] // lanes
    ff_rows = w_down.shape[0]
    unit = ff_rows // lanes
    own_ff = unit * planes
    scale = HEAD_DIM ** (-0.5)

    inputs = lax.all_gather(tokens[0], "dp", axis=0, tiled=True)
    upstream = lax.all_gather(cotangent[0], "dp", axis=0, tiled=True)
    table = lax.all_gather(block_order[0], "dp", axis=0, tiled=False)
    gains = lax.all_gather(jnp.stack([attn_gain, mlp_gain]).astype(LOW), "shard", axis=1, tiled=True)
    gain_one, gain_two = gains[0].astype(FULL), gains[1].astype(FULL)

    def columns(weight, start, count):
        return lax.dynamic_slice_in_dim(weight, start, count, 1).astype(LOW)

    attn_piece = jnp.concatenate(
        [
            columns(w_query, lane * head_cols, head_cols),
            columns(w_key, kv_head * HEAD_DIM, HEAD_DIM),
            columns(w_value, kv_head * HEAD_DIM, HEAD_DIM),
            columns(w_out, lane * out_cols, out_cols),
        ],
        axis=1,
    )
    attn_mat = assemble(plane_parts(attn_piece))
    qkv_cols = head_cols + 2 * HEAD_DIM
    qkv_mat = attn_mat[:, :qkv_cols]
    out_mat = attn_mat[:, qkv_cols:]

    mlp_piece = jnp.concatenate(
        [
            columns(weight, p * ff_rows + lane * unit, unit)
            for weight in (w_gate, w_up)
            for p in range(planes)
        ],
        axis=1,
    )
    mlp_mat = assemble(plane_parts(mlp_piece))
    down_piece = lax.dynamic_slice_in_dim(w_down, lane * unit, unit, 0).astype(LOW)
    down_mat = assemble(plane_parts(down_piece))

    first_row = lane * head_cols
    owner = first_row // own_width
    row_piece = lax.dynamic_slice_in_dim(w_out, first_row - owner * own_width, head_cols, 0).astype(
        LOW
    )
    out_rows = jnp.where(owner == plane, row_piece, jnp.zeros_like(row_piece))
    for k in range(1, planes):
        pairs = []
        for d in range(lanes):
            source = (d * head_cols) // own_width
            pairs.append((d * planes + source, d * planes + (source + k) % planes))
        out_rows = out_rows + lax.ppermute(row_piece, ("dp", "shard"), pairs)

    query_places = places_of(table, plane, rows, span)
    frequency = ROPE_BASE ** (
        -(jnp.arange(HEAD_DIM // 2, dtype=FULL) * 2.0) / HEAD_DIM
    )
    angles = frequency[:, None] * query_places.reshape(-1).astype(FULL)[None, :]
    cosine, sine = jnp.cos(angles), jnp.sin(angles)

    wide = inputs.astype(FULL)
    scale_one = lax.rsqrt(jnp.mean(wide * wide, axis=-1, keepdims=True) + EPSILON)
    hidden_one = (wide * scale_one * gain_one).astype(LOW)
    qkv = contract(qkv_mat, hidden_one, 0, 1)
    query = rope(qkv[:head_cols].reshape(own_heads, HEAD_DIM, total_rows), cosine, sine)
    query = query.astype(LOW)
    key = rope(qkv[head_cols : head_cols + HEAD_DIM], cosine, sine).astype(LOW)
    value = qkv[head_cols + HEAD_DIM :].astype(LOW)
    kv_parts = plane_parts(jnp.concatenate([key, value], axis=0))
    key_places = jnp.concatenate(
        [places_of(table, lax.rem(plane - k + planes, planes), rows, span) for k in range(planes)],
        axis=1,
    )
    kv_all = jnp.stack(kv_parts, axis=0).reshape(planes, 2, HEAD_DIM, seqs, rows)
    kv_all = jnp.transpose(kv_all, (1, 3, 0, 4, 2)).reshape(2, seqs, planes * rows, HEAD_DIM)
    key_all, value_all = kv_all[0], kv_all[1]
    query_heads = jnp.transpose(
        query.reshape(own_heads, HEAD_DIM, seqs, rows), (2, 0, 3, 1)
    )
    visible = (key_places[:, :, None] <= query_places[:, None, :])[:, None]
    scores = (
        jnp.einsum("shqd,skd->shkq", query_heads, key_all, preferred_element_type=FULL) * scale
    )
    scores = jnp.where(visible, scores, MASKED)
    top = jnp.max(scores, axis=2, keepdims=True)
    weights = jnp.exp(scores - top)
    total = jnp.sum(weights, axis=2, keepdims=True)
    probability = weights / total
    log_total = top + jnp.log(total)
    attended = jnp.einsum(
        "shkq,skd->hdsq", probability.astype(LOW), value_all, preferred_element_type=FULL
    ).reshape(head_cols, total_rows)

    attended_all = lax.all_gather(attended.astype(LOW), "dp", axis=0, tiled=True)
    branch = contract(out_mat, attended_all, 0, 0)
    own_inputs = lax.dynamic_slice_in_dim(inputs, lane * out_cols, out_cols, 1)
    middle_part = (own_inputs.astype(FULL).T + branch).astype(LOW)
    middle = lax.all_gather(middle_part, "dp", axis=0, tiled=True)
    wide_two = middle.astype(FULL)
    scale_two = lax.rsqrt(jnp.mean(wide_two * wide_two, axis=0, keepdims=True) + EPSILON)
    hidden_two = (wide_two * scale_two * gain_two[:, None]).astype(LOW)
    both = contract(mlp_mat, hidden_two, 0, 0)
    gate_value, up_value = both[:own_ff], both[own_ff:]
    sigmoid = jax.nn.sigmoid(gate_value)
    silu = gate_value * sigmoid
    inner = (silu * up_value).astype(LOW)

    inner_grad = contract(down_mat, upstream, 1, 1)
    gate_grad = inner_grad * up_value * sigmoid * (1.0 + gate_value * (1.0 - sigmoid))
    up_grad = inner_grad * silu
    both_grad = jnp.concatenate([gate_grad.astype(LOW), up_grad.astype(LOW)], axis=0)
    hidden_two_grad = contract(both_grad, mlp_mat, 0, 1).astype(LOW)
    hidden_two_own = lax.psum_scatter(
        hidden_two_grad, "dp", scatter_dimension=0, tiled=True
    ).astype(FULL)
    middle_own = lax.dynamic_slice_in_dim(middle, lane * rows, rows, 1).astype(FULL).T
    scale_own = lax.rsqrt(jnp.mean(middle_own * middle_own, axis=-1, keepdims=True) + EPSILON)
    middle_norm_grad, gain_two_grad = norm_back(
        hidden_two_own, middle_own * scale_own, scale_own, gain_two
    )
    middle_grad = middle_norm_grad + cotangent[0].astype(FULL)
    branch_grad = lax.all_gather(middle_grad.astype(LOW), "dp", axis=0, tiled=True)

    result = lax.psum_scatter(
        contract(inner, down_mat, 0, 0).astype(LOW), "dp", scatter_dimension=0, tiled=True
    )
    block_out = (middle_own + result.astype(FULL)).astype(LOW)[None]

    mlp_grad = plane_scatter(contract(hidden_two, both_grad, 1, 1))
    down_grad = plane_scatter(contract(inner, upstream, 1, 0))

    attended_grad = contract(out_rows, branch_grad, 1, 1)
    attended_grad_low = attended_grad.astype(LOW)
    grad_heads = attended_grad_low.reshape(own_heads, HEAD_DIM, seqs, rows)
    delta = jnp.sum(
        (attended * attended_grad_low.astype(FULL)).reshape(own_heads, HEAD_DIM, seqs, rows), axis=1
    )
    delta = jnp.transpose(delta, (1, 0, 2))[:, :, None, :]
    grad_heads = jnp.transpose(grad_heads, (2, 0, 3, 1))
    scores = (
        jnp.einsum("shqd,skd->shkq", query_heads, key_all, preferred_element_type=FULL) * scale
    )
    probability = jnp.exp(jnp.where(visible, scores - log_total, MASKED))
    prob_grad = jnp.einsum("shqd,skd->shkq", grad_heads, value_all, preferred_element_type=FULL)
    score_grad = (probability * (prob_grad - delta)).astype(LOW)
    query_grad = (
        jnp.einsum("shkq,skd->hdsq", score_grad, key_all, preferred_element_type=FULL) * scale
    ).reshape(own_heads, HEAD_DIM, total_rows)
    key_grad = (
        jnp.einsum("shkq,shqd->dsk", score_grad, query_heads, preferred_element_type=FULL) * scale
    )
    value_grad = jnp.einsum(
        "shkq,shqd->dsk", probability.astype(LOW), grad_heads, preferred_element_type=FULL
    )
    kv_grad = jnp.concatenate([key_grad, value_grad], axis=0).astype(LOW)
    kv_grad = kv_grad.reshape(2 * HEAD_DIM, seqs, planes, rows)
    kv_own = kv_grad[:, :, 0].astype(FULL)
    for k in range(1, planes):
        kv_own = kv_own + shift(kv_grad[:, :, k], planes - k).astype(FULL)
    kv_own = kv_own.reshape(2 * HEAD_DIM, total_rows)
    query_lin = rope(query_grad, cosine, -sine).astype(LOW).reshape(head_cols, total_rows)
    key_lin = rope(kv_own[:HEAD_DIM], cosine, -sine).astype(LOW)
    qkv_lin = jnp.concatenate([query_lin, key_lin, kv_own[HEAD_DIM:].astype(LOW)], axis=0)
    hidden_one_grad = lax.psum_scatter(
        contract(qkv_lin, qkv_mat, 0, 1).astype(LOW), "dp", scatter_dimension=0, tiled=True
    ).astype(FULL)
    own_tokens = tokens[0].astype(FULL)
    own_scale = lax.rsqrt(jnp.mean(own_tokens * own_tokens, axis=-1, keepdims=True) + EPSILON)
    input_norm_grad, gain_one_grad = norm_back(
        hidden_one_grad, own_tokens * own_scale, own_scale, gain_one
    )
    tokens_grad = (middle_grad + input_norm_grad)[None]

    branch_cols = lax.dynamic_slice_in_dim(branch_grad, lane * out_cols, out_cols, 1)
    attn_grad = jnp.concatenate(
        [
            contract(hidden_one, qkv_lin, 0, 1).astype(LOW),
            contract(attended_all, branch_cols, 1, 0).astype(LOW),
        ],
        axis=1,
    )
    attn_grad = plane_scatter(attn_grad)

    gain_sum = lax.psum(jnp.stack([gain_one_grad, gain_two_grad]), ("dp", "shard"))
    gain_own = lax.dynamic_slice_in_dim(gain_sum, plane * own_width, own_width, 1)

    mlp_all = lax.all_gather(mlp_grad.astype(LOW), "dp", axis=0, tiled=True)
    down_all = lax.all_gather(down_grad.astype(LOW), "dp", axis=0, tiled=True)
    attn_all = lax.all_gather(attn_grad.astype(LOW), "dp", axis=0, tiled=True)

    mlp_all = mlp_all.reshape(lanes, own_width, 2, planes, unit)
    mlp_all = jnp.transpose(mlp_all, (2, 1, 3, 0, 4)).reshape(2, own_width, -1).astype(FULL)
    attn_all = attn_all.reshape(lanes, own_width, -1)
    query_out = jnp.transpose(attn_all[:, :, :head_cols], (1, 0, 2)).reshape(own_width, -1)
    out_out = jnp.transpose(attn_all[:, :, qkv_cols:], (1, 0, 2)).reshape(own_width, -1)
    kv_out = attn_all[:, :, head_cols:qkv_cols].astype(FULL)
    kv_out = kv_out.reshape(kv_heads, lanes // kv_heads, own_width, 2, HEAD_DIM).sum(axis=1)
    kv_out = jnp.transpose(kv_out, (2, 1, 0, 3)).reshape(2, own_width, -1)
    return (
        block_out,
        tokens_grad,
        gain_own[0],
        query_out.astype(FULL),
        kv_out[0],
        kv_out[1],
        out_out.astype(FULL),
        gain_own[1],
        mlp_all[0],
        mlp_all[1],
        down_all.astype(FULL),
    )


def solution(mesh):
    rows = P("shard", None)
    acts = P("dp", "shard", None)
    gain = P("shard")
    weights = (gain, rows, rows, rows, rows, gain, rows, rows, rows)
    return jax.shard_map(
        on_device,
        mesh=mesh,
        in_specs=(acts, P("dp", None)) + weights + (acts,),
        out_specs=(acts, acts) + weights,
        check_vma=False,
    )
```

```python
import functools

import jax
import jax.numpy as jnp
from jax import lax
from jax.experimental import pallas as pl
from jax.sharding import PartitionSpec as P

HEAD_DIM = 64
EPSILON = 1e-05
ROPE_BASE = 10000.0
MASKED = -1e30
LOW = jnp.bfloat16
FULL = jnp.float32
EXTRA = 32


def contract(left, right, left_dim, right_dim):
    return lax.dot_general(
        left, right, (((left_dim,), (right_dim,)), ((), ())), preferred_element_type=FULL
    )


def shift(value, amount):
    count = lax.axis_size("shard")
    pairs = [(i, (i + amount) % count) for i in range(count)]
    return lax.ppermute(value, "shard", pairs)


def plane_parts(value):
    count = lax.axis_size("shard")
    return [value] + [shift(value, k) for k in range(1, count)]


def assemble(parts, axis=0):
    count = lax.axis_size("shard")
    rank = lax.axis_index("shard")
    rows = parts[0].shape[axis]
    shape = list(parts[0].shape)
    shape[axis] = rows * count
    whole = jnp.zeros(shape, parts[0].dtype)
    for k, part in enumerate(parts):
        place = lax.rem(rank - k + count, count)
        whole = lax.dynamic_update_slice_in_dim(whole, part, place * rows, axis)
    return whole


def plane_send(value):
    count = lax.axis_size("shard")
    rank = lax.axis_index("shard")
    rows = value.shape[0] // count
    parts = []
    for k in range(count):
        target = lax.rem(rank + k, count)
        piece = lax.dynamic_slice_in_dim(value, target * rows, rows, 0)
        parts.append(shift(piece, k) if k else piece)
    return parts


def plane_sum(parts):
    total = parts[0].astype(FULL)
    for part in parts[1:]:
        total = total + part.astype(FULL)
    return total.astype(LOW)


def rope(values, cosine, sine):
    half = values.shape[-2] // 2
    front, back = values[..., :half, :], values[..., half:, :]
    return jnp.concatenate([front * cosine - back * sine, back * cosine + front * sine], axis=-2)


def places_of(table, plane, rows, span):
    blocks = rows // span
    count = table.shape[1] // blocks
    grouped = table.reshape(table.shape[0], count, blocks)
    picked = lax.dynamic_slice_in_dim(grouped, plane, 1, 1)[:, 0]
    within = jnp.arange(span, dtype=jnp.int32)
    return (picked[:, :, None] * span + within[None, None, :]).reshape(table.shape[0], rows)


def spread_kernel(lanes, planes, unit, piece_ref, gate_ref, up_ref):
    for which, out_ref in enumerate((gate_ref, up_ref)):
        for p in range(planes):
            for d in range(lanes):
                start = (which * planes + p) * unit
                place = (p * lanes + d) * unit
                out_ref[:, place : place + unit] = piece_ref[d, :, start : start + unit].astype(FULL)


def spread_mlp(pieces, planes, unit):
    lanes, rows, cols = pieces.shape
    block = min(64, rows)
    full = jax.ShapeDtypeStruct((rows, lanes * planes * unit), FULL)
    spec = pl.BlockSpec((block, lanes * planes * unit), lambda i: (i, 0))
    return pl.pallas_call(
        functools.partial(spread_kernel, lanes, planes, unit),
        out_shape=(full, full),
        grid=(rows // block,),
        in_specs=[pl.BlockSpec((lanes, block, cols), lambda i: (0, i, 0))],
        out_specs=(spec, spec),
        cost_estimate=pl.CostEstimate(
            flops=0, bytes_accessed=lanes * rows * cols * 6, transcendentals=0
        ),
    )(pieces)


def gather_kernel(lanes, head_cols, out_cols, sharing, piece_ref, q_ref, k_ref, v_ref, o_ref):
    first_key, first_value = head_cols, head_cols + HEAD_DIM
    first_out = head_cols + 2 * HEAD_DIM
    for d in range(lanes):
        q_ref[:, d * head_cols : (d + 1) * head_cols] = piece_ref[d, :, :head_cols].astype(FULL)
        o_ref[:, d * out_cols : (d + 1) * out_cols] = piece_ref[d, :, first_out:].astype(FULL)
    for h in range(lanes // sharing):
        for start, out_ref in ((first_key, k_ref), (first_value, v_ref)):
            total = None
            for d in range(h * sharing, (h + 1) * sharing):
                part = piece_ref[d, :, start : start + HEAD_DIM].astype(FULL)
                total = part if total is None else total + part
            out_ref[:, h * HEAD_DIM : (h + 1) * HEAD_DIM] = total


def spread_attn(pieces, rows, head_cols, out_cols, kv_heads):
    lanes, _, cols = pieces.shape
    widths = (lanes * head_cols, kv_heads * HEAD_DIM, kv_heads * HEAD_DIM, lanes * out_cols)
    return pl.pallas_call(
        functools.partial(gather_kernel, lanes, head_cols, out_cols, lanes // kv_heads),
        out_shape=tuple(jax.ShapeDtypeStruct((rows, w), FULL) for w in widths),
        grid=(rows // EXTRA,),
        in_specs=[pl.BlockSpec((lanes, EXTRA, cols), lambda i: (0, i, 0))],
        out_specs=tuple(pl.BlockSpec((EXTRA, w), lambda i: (i, 0)) for w in widths),
        cost_estimate=pl.CostEstimate(
            flops=0, bytes_accessed=lanes * rows * cols * 6, transcendentals=0
        ),
    )(pieces)


def norm_back(upstream, normed, row_scale, gain):
    scaled = upstream * gain
    gain_grad = jnp.sum(upstream * normed, axis=0)
    mean = jnp.mean(scaled * normed, axis=-1, keepdims=True)
    return row_scale * (scaled - normed * mean), gain_grad


def on_device(
    tokens,
    block_order,
    attn_gain,
    w_query,
    w_key,
    w_value,
    w_out,
    mlp_gain,
    w_gate,
    w_up,
    w_down,
    cotangent,
):
    planes = lax.axis_size("shard")
    plane = lax.axis_index("shard")
    lanes = lax.axis_size("dp")
    lane = lax.axis_index("dp")
    rows = tokens.shape[1]
    width = tokens.shape[2]
    span = rows // 2
    seqs = lanes
    total_rows = seqs * rows
    own_width = width // planes
    heads = w_query.shape[1] // HEAD_DIM
    kv_heads = w_key.shape[1] // HEAD_DIM
    own_heads = heads // lanes
    head_cols = own_heads * HEAD_DIM
    kv_head = (lane * own_heads * kv_heads) // heads
    out_cols = w_out.shape[1] // lanes
    ff_rows = w_down.shape[0]
    unit = ff_rows // lanes
    own_ff = unit * planes
    scale = HEAD_DIM ** (-0.5)

    inputs = lax.all_gather(tokens[0], "dp", axis=0, tiled=True)
    upstream = lax.all_gather(cotangent[0], "dp", axis=0, tiled=True)
    table = lax.all_gather(block_order[0], "dp", axis=0, tiled=False)

    def columns(weight, start, count):
        return lax.dynamic_slice_in_dim(weight, start, count, 1).astype(LOW)

    attn_piece = jnp.concatenate(
        [
            columns(w_query, lane * head_cols, head_cols),
            columns(w_key, kv_head * HEAD_DIM, HEAD_DIM),
            columns(w_value, kv_head * HEAD_DIM, HEAD_DIM),
            columns(w_out, lane * out_cols, out_cols),
        ],
        axis=1,
    )
    piece_cols = attn_piece.shape[1]
    gain_rows = jnp.stack([attn_gain, mlp_gain]).astype(LOW)
    gain_rows = jnp.pad(gain_rows, ((0, EXTRA - 2), (0, piece_cols - own_width)))
    attn_parts = plane_parts(jnp.concatenate([attn_piece, gain_rows], axis=0))
    attn_mat = assemble([part[:own_width] for part in attn_parts])
    gains = assemble([part[own_width : own_width + 2, :own_width] for part in attn_parts], 1)
    gain_one, gain_two = gains[0].astype(FULL), gains[1].astype(FULL)
    qkv_cols = head_cols + 2 * HEAD_DIM
    qkv_mat = attn_mat[:, :qkv_cols]
    out_mat = attn_mat[:, qkv_cols:]

    mlp_piece = jnp.concatenate(
        [
            columns(weight, p * ff_rows + lane * unit, unit)
            for weight in (w_gate, w_up)
            for p in range(planes)
        ],
        axis=1,
    )
    mlp_parts = plane_parts(mlp_piece)
    mlp_mat = assemble(mlp_parts)
    down_piece = lax.dynamic_slice_in_dim(w_down, lane * unit, unit, 0).astype(LOW)
    down_parts = plane_parts(down_piece)
    down_mat = assemble(down_parts)

    first_row = lane * head_cols
    owner = first_row // own_width
    row_piece = lax.dynamic_slice_in_dim(w_out, first_row - owner * own_width, head_cols, 0).astype(
        LOW
    )
    out_rows = jnp.where(owner == plane, row_piece, jnp.zeros_like(row_piece))
    for k in range(1, planes):
        pairs = []
        for d in range(lanes):
            source = (d * head_cols) // own_width
            pairs.append((d * planes + source, d * planes + (source + k) % planes))
        out_rows = out_rows + lax.ppermute(row_piece, ("dp", "shard"), pairs)

    query_places = places_of(table, plane, rows, span)
    frequency = ROPE_BASE ** (
        -(jnp.arange(HEAD_DIM // 2, dtype=FULL) * 2.0) / HEAD_DIM
    )
    angles = frequency[:, None] * query_places.reshape(-1).astype(FULL)[None, :]
    cosine, sine = jnp.cos(angles), jnp.sin(angles)

    wide = inputs.astype(FULL)
    scale_one = lax.rsqrt(jnp.mean(wide * wide, axis=-1, keepdims=True) + EPSILON)
    hidden_one = (wide * scale_one * gain_one).astype(LOW)
    qkv = contract(qkv_mat, hidden_one, 0, 1)
    query = rope(qkv[:head_cols].reshape(own_heads, HEAD_DIM, total_rows), cosine, sine)
    query = query.astype(LOW)
    key = rope(qkv[head_cols : head_cols + HEAD_DIM], cosine, sine).astype(LOW)
    value = qkv[head_cols + HEAD_DIM :].astype(LOW)
    kv_parts = plane_parts(jnp.concatenate([key, value], axis=0))
    key_places = jnp.concatenate(
        [places_of(table, lax.rem(plane - k + planes, planes), rows, span) for k in range(planes)],
        axis=1,
    )
    kv_all = jnp.stack(kv_parts, axis=0).reshape(planes, 2, HEAD_DIM, seqs, rows)
    kv_all = jnp.transpose(kv_all, (1, 3, 0, 4, 2)).reshape(2, seqs, planes * rows, HEAD_DIM)
    key_all, value_all = kv_all[0], kv_all[1]
    query_heads = jnp.transpose(
        query.reshape(own_heads, HEAD_DIM, seqs, rows), (2, 0, 3, 1)
    )
    visible = (key_places[:, :, None] <= query_places[:, None, :])[:, None]
    scores = (
        jnp.einsum("shqd,skd->shkq", query_heads, key_all, preferred_element_type=FULL) * scale
    )
    scores = jnp.where(visible, scores, MASKED)
    top = jnp.max(scores, axis=2, keepdims=True)
    weights = jnp.exp(scores - top)
    total = jnp.sum(weights, axis=2, keepdims=True)
    probability = weights / total
    log_total = top + jnp.log(total)
    attended = jnp.einsum(
        "shkq,skd->hdsq", probability.astype(LOW), value_all, preferred_element_type=FULL
    ).reshape(head_cols, total_rows)

    attended_all = lax.all_gather(attended.astype(LOW), "dp", axis=0, tiled=True)
    branch = contract(out_mat, attended_all, 0, 0)
    own_inputs = lax.dynamic_slice_in_dim(inputs, lane * out_cols, out_cols, 1)
    middle_part = (own_inputs.astype(FULL).T + branch).astype(LOW)
    middle = lax.all_gather(middle_part, "dp", axis=0, tiled=True)
    wide_two = middle.astype(FULL)
    scale_two = lax.rsqrt(jnp.mean(wide_two * wide_two, axis=0, keepdims=True) + EPSILON)
    hidden_two = (wide_two * scale_two * gain_two[:, None]).astype(LOW)
    both = contract(mlp_mat, hidden_two, 0, 0)
    gate_value, up_value = both[:own_ff], both[own_ff:]
    sigmoid = jax.nn.sigmoid(gate_value)
    silu = gate_value * sigmoid
    inner = (silu * up_value).astype(LOW)

    inner_grad = contract(down_mat, upstream, 1, 1)
    gate_grad = inner_grad * up_value * sigmoid * (1.0 + gate_value * (1.0 - sigmoid))
    up_grad = inner_grad * silu
    both_grad = jnp.concatenate([gate_grad.astype(LOW), up_grad.astype(LOW)], axis=0)
    hidden_two_grad = contract(both_grad, mlp_mat, 0, 1).astype(LOW)
    hidden_two_own = lax.psum_scatter(hidden_two_grad, "dp", scatter_dimension=0, tiled=True)
    mlp_grad = contract(hidden_two, both_grad, 1, 1).astype(LOW)
    down_grad = contract(inner, upstream, 1, 0).astype(LOW)
    mlp_sent = plane_send(mlp_grad)
    down_sent = plane_send(down_grad)
    partial_out = contract(inner, down_mat, 0, 0).astype(LOW)
    hidden_two_own = hidden_two_own.astype(FULL)
    middle_own = lax.dynamic_slice_in_dim(middle, lane * rows, rows, 1).astype(FULL).T
    scale_own = lax.rsqrt(jnp.mean(middle_own * middle_own, axis=-1, keepdims=True) + EPSILON)
    middle_norm_grad, gain_two_grad = norm_back(
        hidden_two_own, middle_own * scale_own, scale_own, gain_two
    )
    middle_grad = middle_norm_grad + cotangent[0].astype(FULL)
    middle_grad_low = middle_grad.astype(LOW)
    branch_grad = lax.all_gather(middle_grad_low, "dp", axis=0, tiled=True)

    partial_out, branch_grad = lax.optimization_barrier((partial_out, branch_grad))
    result = lax.psum_scatter(partial_out, "dp", scatter_dimension=0, tiled=True)
    block_out = (middle_own + result.astype(FULL)).astype(LOW)[None]

    attended_grad = contract(out_rows, branch_grad, 1, 1)
    attended_grad_low = attended_grad.astype(LOW)
    grad_heads = attended_grad_low.reshape(own_heads, HEAD_DIM, seqs, rows)
    delta = jnp.sum(
        (attended * attended_grad_low.astype(FULL)).reshape(own_heads, HEAD_DIM, seqs, rows), axis=1
    )
    delta = jnp.transpose(delta, (1, 0, 2))[:, :, None, :]
    grad_heads = jnp.transpose(grad_heads, (2, 0, 3, 1))
    scores = (
        jnp.einsum("shqd,skd->shkq", query_heads, key_all, preferred_element_type=FULL) * scale
    )
    probability = jnp.exp(jnp.where(visible, scores - log_total, MASKED))
    prob_grad = jnp.einsum("shqd,skd->shkq", grad_heads, value_all, preferred_element_type=FULL)
    score_grad = (probability * (prob_grad - delta)).astype(LOW)
    query_grad = (
        jnp.einsum("shkq,skd->hdsq", score_grad, key_all, preferred_element_type=FULL) * scale
    ).reshape(own_heads, HEAD_DIM, total_rows)
    key_grad = (
        jnp.einsum("shkq,shqd->dsk", score_grad, query_heads, preferred_element_type=FULL) * scale
    )
    value_grad = jnp.einsum(
        "shkq,shqd->dsk", probability.astype(LOW), grad_heads, preferred_element_type=FULL
    )

    kv_grad = jnp.concatenate([key_grad, value_grad], axis=0).astype(LOW)
    kv_grad = kv_grad.reshape(2 * HEAD_DIM, seqs, planes, rows)
    kv_own = kv_grad[:, :, 0].astype(FULL)
    for k in range(1, planes):
        part = shift(kv_grad[:, :, k], planes - k)
        kv_own = kv_own + part.astype(FULL)
    kv_own = kv_own.reshape(2 * HEAD_DIM, total_rows)
    query_lin = rope(query_grad, cosine, -sine).astype(LOW).reshape(head_cols, total_rows)
    key_lin = rope(kv_own[:HEAD_DIM], cosine, -sine).astype(LOW)
    qkv_lin = jnp.concatenate([query_lin, key_lin, kv_own[HEAD_DIM:].astype(LOW)], axis=0)
    hidden_one_part = contract(qkv_lin, qkv_mat, 0, 1)
    hidden_one_low = hidden_one_part.astype(LOW)
    hidden_one_grad = lax.psum_scatter(
        hidden_one_low, "dp", scatter_dimension=0, tiled=True
    ).astype(FULL)
    gain_one_grad = jnp.sum(hidden_one_low.astype(FULL) * (wide * scale_one), axis=0)
    own_tokens = tokens[0].astype(FULL)
    own_scale = lax.rsqrt(jnp.mean(own_tokens * own_tokens, axis=-1, keepdims=True) + EPSILON)
    input_norm_grad, _ = norm_back(
        hidden_one_grad, own_tokens * own_scale, own_scale, gain_one
    )
    tokens_grad = (middle_grad + input_norm_grad)[None]

    branch_cols = lax.dynamic_slice_in_dim(branch_grad, lane * out_cols, out_cols, 1)
    qkv_grad = contract(hidden_one, qkv_lin, 0, 1).astype(LOW)
    out_grad = contract(attended_all, branch_cols, 1, 0).astype(LOW)
    attn_grad = jnp.concatenate([qkv_grad, out_grad], axis=1).reshape(planes, own_width, -1)
    gain_grads = jnp.stack([gain_one_grad, gain_two_grad]).astype(LOW)
    gain_grads = jnp.transpose(gain_grads.reshape(2, planes, own_width), (1, 0, 2))
    gain_grads = jnp.pad(gain_grads, ((0, 0), (0, EXTRA - 2), (0, piece_cols - own_width)))
    attn_grad = jnp.concatenate([attn_grad, gain_grads], axis=1)
    attn_sent = plane_send(attn_grad.reshape(-1, piece_cols))

    mlp_all = lax.all_gather(plane_sum(mlp_sent), "dp", axis=0, tiled=False)
    down_all = lax.all_gather(plane_sum(down_sent), "dp", axis=0, tiled=True)
    attn_all = lax.all_gather(plane_sum(attn_sent), "dp", axis=0, tiled=False)

    gate_out, up_out = spread_mlp(mlp_all, planes, unit)
    query_out, key_out, value_out, out_out = spread_attn(
        attn_all, own_width, head_cols, out_cols, kv_heads
    )
    gain_own = jnp.sum(attn_all[:, own_width : own_width + 2, :own_width].astype(FULL), axis=0)
    return (
        block_out,
        tokens_grad,
        gain_own[0],
        query_out,
        key_out,
        value_out,
        out_out,
        gain_own[1],
        gate_out,
        up_out,
        down_all.astype(FULL),
    )


def solution(mesh):
    rows = P("shard", None)
    acts = P("dp", "shard", None)
    gain = P("shard")
    weights = (gain, rows, rows, rows, rows, gain, rows, rows, rows)

    return jax.shard_map(
        on_device,
        mesh=mesh,
        in_specs=(acts, P("dp", None)) + weights + (acts,),
        out_specs=(acts, acts) + weights,
        check_vma=False,
    )
```

```python
import functools

import jax
import jax.numpy as jnp
from jax import lax
from jax.experimental import pallas as pl
from jax.experimental.pallas import tpu as pltpu
from jax.sharding import PartitionSpec as P

HEAD_DIM = 64
EPSILON = 1e-05
ROPE_BASE = 10000.0
MASKED = -1e30
LOW = jnp.bfloat16
FULL = jnp.float32
EXTRA = 32


def contract(left, right, left_dim, right_dim):
    return lax.dot_general(
        left, right, (((left_dim,), (right_dim,)), ((), ())), preferred_element_type=FULL
    )


def shift(value, amount):
    count = lax.axis_size("shard")
    pairs = [(i, (i + amount) % count) for i in range(count)]
    return lax.ppermute(value, "shard", pairs)


def swap_cores(value):
    lanes = lax.axis_size("dp")
    return lax.ppermute(value, "dp", [(d, d ^ 1) for d in range(lanes)])


def swap_chips(value, mask):
    lanes = lax.axis_size("dp")
    return lax.ppermute(value, "dp", [(d, d ^ (2 * mask)) for d in range(lanes)])


def plane_parts(value):
    count = lax.axis_size("shard")
    return [value] + [shift(value, k) for k in range(1, count)]


def assemble(parts, axis=0):
    count = lax.axis_size("shard")
    rank = lax.axis_index("shard")
    rows = parts[0].shape[axis]
    shape = list(parts[0].shape)
    shape[axis] = rows * count
    whole = jnp.zeros(shape, parts[0].dtype)
    for k, part in enumerate(parts):
        place = lax.rem(rank - k + count, count)
        whole = lax.dynamic_update_slice_in_dim(whole, part, place * rows, axis)
    return whole


def plane_send(value):
    count = lax.axis_size("shard")
    rank = lax.axis_index("shard")
    rows = value.shape[0] // count
    parts = []
    for k in range(count):
        target = lax.rem(rank + k, count)
        piece = lax.dynamic_slice_in_dim(value, target * rows, rows, 0)
        parts.append(shift(piece, k) if k else piece)
    return parts


def plane_sum(parts):
    total = parts[0].astype(FULL)
    for part in parts[1:]:
        total = total + part.astype(FULL)
    return total.astype(LOW)


def chip_stack(value):
    chips = lax.axis_size("dp") // 2
    return [value] + [swap_chips(value, k) for k in range(1, chips)]


def rope(values, cosine, sine):
    half = values.shape[-2] // 2
    front, back = values[..., :half, :], values[..., half:, :]
    return jnp.concatenate([front * cosine - back * sine, back * cosine + front * sine], axis=-2)


def norm_back(upstream, normed, row_scale, gain):
    scaled = upstream * gain
    mean = jnp.mean(scaled * normed, axis=-1, keepdims=True)
    return row_scale * (scaled - normed * mean)


class Tiles:
    def __init__(self, info_ref, planes, span, heads):
        self.info, self.planes, self.span, self.heads = info_ref, planes, span, heads
        self.seq = pl.program_id(0)

    def offset(self, part, high):
        first = self.info[self.seq, part]
        return pl.multiple_of(jnp.where(first == high, 0, 1) * self.span, self.span)

    def before(self, part):
        return self.info[self.seq, self.planes + part] == 1

    def picked(self, part, own):
        return jnp.where(self.before(part), self.offset(own, 0), self.offset(own, 1))

    def heads_of(self, ref, offset):
        offset = pl.multiple_of(offset, self.span)
        rows = [
            ref[h * HEAD_DIM : (h + 1) * HEAD_DIM, pl.ds(offset, self.span)]
            for h in range(self.heads)
        ]
        return jnp.concatenate(rows, axis=1)

    def put_heads(self, ref, offset, value):
        for h in range(self.heads):
            piece = value[:, h * self.span : (h + 1) * self.span]
            ref[h * HEAD_DIM : (h + 1) * HEAD_DIM, pl.ds(offset, self.span)] = piece.astype(
                ref.dtype
            )

    def block(self, ref, part, offset):
        return ref[part, :, pl.ds(pl.multiple_of(offset, self.span), self.span)]

    def diagonal(self):
        shape = (self.span, self.heads * self.span)
        keys = lax.broadcasted_iota(jnp.int32, shape, 0)
        queries = lax.broadcasted_iota(jnp.int32, shape, 1)
        return keys <= lax.rem(queries, self.span)


def top_of(value):
    return jnp.max(value, axis=0, keepdims=True)


def sum_of(value):
    return jnp.sum(value, axis=0, keepdims=True)


def attn_fwd_kernel(planes, span, heads, info_ref, q_ref, k_ref, v_ref, o_ref, lse_ref):
    tiles = Tiles(info_ref, planes, span, heads)
    low_at, high_at = tiles.offset(0, 0), tiles.offset(0, 1)
    q_low, q_high = tiles.heads_of(q_ref, low_at), tiles.heads_of(q_ref, high_at)
    visible = tiles.diagonal()

    def score(part, offset, query):
        return contract(tiles.block(k_ref, part, offset), query, 0, 0)

    own_low = jnp.where(visible, score(0, low_at, q_low), MASKED)
    own_high = jnp.where(visible, score(0, high_at, q_high), MASKED)
    wide = [score(p, tiles.offset(p, 0), q_high) for p in range(planes)]
    mixed = []
    for p in range(1, planes):
        query = tiles.heads_of(q_ref, tiles.picked(p, 0))
        mixed.append(score(p, tiles.picked(p, p), query))
    top_low, top_high = top_of(own_low), top_of(own_high)
    for value in wide:
        top_high = jnp.maximum(top_high, top_of(value))
    for p in range(1, planes):
        peak = top_of(mixed[p - 1])
        top_low = jnp.maximum(top_low, jnp.where(tiles.before(p), peak, MASKED))
        top_high = jnp.maximum(top_high, jnp.where(tiles.before(p), MASKED, peak))

    def add(part, offset, value, top):
        weight = jnp.exp(value - top)
        block = tiles.block(v_ref, part, offset)
        return sum_of(weight), contract(block, weight.astype(LOW), 1, 0)

    total_low, out_low = add(0, low_at, own_low, top_low)
    total_high, out_high = add(0, high_at, own_high, top_high)
    for p in range(planes):
        total, out = add(p, tiles.offset(p, 0), wide[p], top_high)
        total_high, out_high = total_high + total, out_high + out
    for p in range(1, planes):
        early = tiles.before(p)
        top = jnp.where(early, top_low, top_high)
        total, out = add(p, tiles.picked(p, p), mixed[p - 1], top)
        total_low = total_low + jnp.where(early, total, 0.0)
        total_high = total_high + jnp.where(early, 0.0, total)
        out_low = out_low + jnp.where(early, out, 0.0)
        out_high = out_high + jnp.where(early, 0.0, out)
    tiles.put_heads(o_ref, low_at, out_low / total_low)
    tiles.put_heads(o_ref, high_at, out_high / total_high)
    lse_ref[0, 0:1, :] = top_low + jnp.log(total_low)
    lse_ref[0, 1:2, :] = top_high + jnp.log(total_high)


def attn_bwd_kernel(
    planes, span, heads, info_ref, q_ref, k_ref, v_ref, o_ref, lse_ref, g_ref, dq_ref, dk_ref, dv_ref
):
    tiles = Tiles(info_ref, planes, span, heads)
    low_at, high_at = tiles.offset(0, 0), tiles.offset(0, 1)
    visible = tiles.diagonal()

    def state(offset, row):
        query, grad = tiles.heads_of(q_ref, offset), tiles.heads_of(g_ref, offset)
        out = tiles.heads_of(o_ref, offset)
        delta = sum_of(out.astype(FULL) * grad.astype(FULL))
        return query, grad, lse_ref[0, row : row + 1, :], delta

    low, high = state(low_at, 0), state(high_at, 1)

    def tile(part, offset, queries, masked=False):
        query, grad, log_total, delta = queries
        key, value = tiles.block(k_ref, part, offset), tiles.block(v_ref, part, offset)
        scores = contract(key, query, 0, 0)
        if masked:
            scores = jnp.where(visible, scores, MASKED)
        weight = jnp.exp(scores - log_total)
        change = contract(value, grad, 0, 0)
        change = (weight * (change - delta)).astype(LOW)
        dq = contract(key, change, 1, 0)
        dk = contract(query, change, 1, 1)
        dv = contract(grad, weight.astype(LOW), 1, 1)
        return dq, dk, dv

    dq_low, dk_low, dv_low = tile(0, low_at, low, True)
    dq_high, dk_high, dv_high = tile(0, high_at, high, True)

    def put(part, offset, dk, dv):
        place = pl.ds(pl.multiple_of(offset, span), span)
        dk_ref[part, :, place] = dk.astype(dk_ref.dtype)
        dv_ref[part, :, place] = dv.astype(dv_ref.dtype)

    put(0, high_at, dk_high, dv_high)
    for p in range(planes):
        dq, dk, dv = tile(p, tiles.offset(p, 0), high)
        dq_high = dq_high + dq
        if p == 0:
            put(0, low_at, dk_low + dk, dv_low + dv)
            continue
        early = tiles.before(p)
        at = tiles.picked(p, 0)
        queries = (
            tiles.heads_of(q_ref, at),
            tiles.heads_of(g_ref, at),
            jnp.where(early, low[2], high[2]),
            jnp.where(early, low[3], high[3]),
        )
        dq, dk_mixed, dv_mixed = tile(p, tiles.picked(p, p), queries)
        dq_low = dq_low + jnp.where(early, dq, 0.0)
        dq_high = dq_high + jnp.where(early, 0.0, dq)
        put(
            p,
            tiles.offset(p, 0),
            dk + jnp.where(early, dk_mixed, 0.0),
            dv + jnp.where(early, dv_mixed, 0.0),
        )
        put(
            p,
            tiles.offset(p, 1),
            jnp.where(early, 0.0, dk_mixed),
            jnp.where(early, 0.0, dv_mixed),
        )
    scale = HEAD_DIM ** (-0.5)
    tiles.put_heads(dq_ref, low_at, dq_low * scale)
    tiles.put_heads(dq_ref, high_at, dq_high * scale)


def attn_specs(planes, rows, cols, heads):
    act = pl.BlockSpec((cols, rows), lambda s, info: (0, s))
    keys = pl.BlockSpec((planes, HEAD_DIM, rows), lambda s, info: (0, 0, s))
    lse = pl.BlockSpec((1, 2, heads * rows // 2), lambda s, info: (s, 0, 0))
    return act, keys, lse


def attn_cost(seqs, planes, rows, cols, dots):
    pairs = seqs * rows * rows // 4 * (2 * planes + 1) * (cols // HEAD_DIM)
    return pl.CostEstimate(
        flops=2 * dots * pairs * HEAD_DIM,
        bytes_accessed=2 * seqs * rows * (3 * cols + 4 * planes * HEAD_DIM),
        transcendentals=pairs,
    )


def attn_forward(info, query, key, value, seqs):
    planes, cols = key.shape[0], query.shape[0]
    rows, heads = query.shape[1] // seqs, cols // HEAD_DIM
    act, keys, lse = attn_specs(planes, rows, cols, heads)
    return pl.pallas_call(
        functools.partial(attn_fwd_kernel, planes, rows // 2, heads),
        out_shape=(
            jax.ShapeDtypeStruct(query.shape, LOW),
            jax.ShapeDtypeStruct((seqs, 2, heads * rows // 2), FULL),
        ),
        grid_spec=pltpu.PrefetchScalarGridSpec(
            num_scalar_prefetch=1,
            grid=(seqs,),
            in_specs=[act, keys, keys],
            out_specs=(act, lse),
        ),
        cost_estimate=attn_cost(seqs, planes, rows, cols, 2),
    )(info, query, key, value)


def attn_backward(info, query, key, value, out, lse_value, grad, seqs):
    planes, cols = key.shape[0], query.shape[0]
    rows, heads = query.shape[1] // seqs, cols // HEAD_DIM
    act, keys, lse = attn_specs(planes, rows, cols, heads)
    return pl.pallas_call(
        functools.partial(attn_bwd_kernel, planes, rows // 2, heads),
        out_shape=(
            jax.ShapeDtypeStruct(query.shape, FULL),
            jax.ShapeDtypeStruct(key.shape, LOW),
            jax.ShapeDtypeStruct(key.shape, LOW),
        ),
        grid_spec=pltpu.PrefetchScalarGridSpec(
            num_scalar_prefetch=1,
            grid=(seqs,),
            in_specs=[act, keys, keys, act, lse, act],
            out_specs=(act, keys, keys),
        ),
        cost_estimate=attn_cost(seqs, planes, rows, cols, 5),
    )(info, query, key, value, out, lse_value, grad)


def picker(lane_ref, mine_ref, other_ref):
    lane = lane_ref[0]
    chip, core = lane // 2, lane % 2

    def pick(d, *index):
        slot = (d // 2) ^ chip
        mine = mine_ref[(slot,) + index].astype(FULL)
        other = other_ref[(slot,) + index].astype(FULL)
        return jnp.where(core == d % 2, mine, other)

    return pick


def spread_mlp_kernel(lanes, planes, unit, lane_ref, mine_ref, other_ref, gate_ref, up_ref):
    pick = picker(lane_ref, mine_ref, other_ref)
    every = slice(None)
    for which, out_ref in enumerate((gate_ref, up_ref)):
        for p in range(planes):
            for d in range(lanes):
                start = (which * planes + p) * unit
                place = (p * lanes + d) * unit
                out_ref[:, place : place + unit] = pick(d, every, slice(start, start + unit))


def spread_attn_kernel(
    lanes, head_cols, out_cols, sharing, lane_ref, mine_ref, other_ref, q_ref, k_ref, v_ref, o_ref
):
    pick = picker(lane_ref, mine_ref, other_ref)
    every = slice(None)
    middle = head_cols + HEAD_DIM
    for d in range(lanes):
        q_ref[:, d * head_cols : (d + 1) * head_cols] = pick(d, every, slice(0, head_cols))
        o_ref[:, d * out_cols : (d + 1) * out_cols] = pick(
            d, every, slice(middle, middle + out_cols)
        )
    for h in range(lanes // sharing):
        for first, out_ref in ((0, k_ref), (1, v_ref)):
            total = None
            for d in range(h * sharing + first, (h + 1) * sharing, 2):
                part = pick(d, every, slice(head_cols, middle))
                total = part if total is None else total + part
            out_ref[:, h * HEAD_DIM : (h + 1) * HEAD_DIM] = total


def spread_down_kernel(lane_ref, mine_ref, other_ref, out_ref):
    core = lane_ref[0] % 2
    mine, other = mine_ref[0].astype(FULL), other_ref[0].astype(FULL)
    out_ref[...] = jnp.where(core == pl.program_id(0) % 2, mine, other)


def spread_call(kernel, lane, mine, other, rows, block, widths):
    chips, _, cols = mine.shape
    spec = pl.BlockSpec((chips, block, cols), lambda i, lane_ref: (0, i, 0))
    return pl.pallas_call(
        kernel,
        out_shape=tuple(jax.ShapeDtypeStruct((rows, w), FULL) for w in widths),
        grid_spec=pltpu.PrefetchScalarGridSpec(
            num_scalar_prefetch=1,
            grid=(rows // block,),
            in_specs=[spec, spec],
            out_specs=tuple(pl.BlockSpec((block, w), lambda i, lane_ref: (i, 0)) for w in widths),
        ),
        cost_estimate=pl.CostEstimate(
            flops=0, bytes_accessed=chips * rows * cols * 12, transcendentals=0
        ),
    )(lane, mine, other)


def spread_down(lane, mine, other):
    chips, rows, cols = mine.shape
    spec = pl.BlockSpec(
        (1, rows, cols), lambda d, lane_ref: ((d // 2) ^ (lane_ref[0] // 2), 0, 0)
    )
    return pl.pallas_call(
        spread_down_kernel,
        out_shape=jax.ShapeDtypeStruct((2 * chips * rows, cols), FULL),
        grid_spec=pltpu.PrefetchScalarGridSpec(
            num_scalar_prefetch=1,
            grid=(2 * chips,),
            in_specs=[spec, spec],
            out_specs=pl.BlockSpec((rows, cols), lambda d, lane_ref: (d, 0)),
        ),
        cost_estimate=pl.CostEstimate(
            flops=0, bytes_accessed=chips * rows * cols * 12, transcendentals=0
        ),
    )(lane, mine, other)


def on_device(
    tokens,
    block_order,
    attn_gain,
    w_query,
    w_key,
    w_value,
    w_out,
    mlp_gain,
    w_gate,
    w_up,
    w_down,
    cotangent,
):
    planes = lax.axis_size("shard")
    plane = lax.axis_index("shard")
    lanes = lax.axis_size("dp")
    lane = lax.axis_index("dp")
    odd = lax.rem(lane, 2) == 1
    rows = tokens.shape[1]
    width = tokens.shape[2]
    span = rows // 2
    seqs = lanes
    total_rows = seqs * rows
    own_width = width // planes
    heads = w_query.shape[1] // HEAD_DIM
    kv_heads = w_key.shape[1] // HEAD_DIM
    own_heads = heads // lanes
    head_cols = own_heads * HEAD_DIM
    kv_head = (lane * own_heads * kv_heads) // heads
    out_cols = w_out.shape[1] // lanes
    ff_rows = w_down.shape[0]
    unit = ff_rows // lanes
    own_ff = unit * planes
    scale = HEAD_DIM ** (-0.5)

    inputs = lax.all_gather(tokens[0], "dp", axis=0, tiled=True)
    upstream = lax.all_gather(cotangent[0], "dp", axis=0, tiled=True)
    table = lax.all_gather(block_order[0], "dp", axis=0, tiled=False)

    def columns(weight, start, count):
        return lax.dynamic_slice_in_dim(weight, start, count, 1).astype(LOW)

    kv_at = kv_head * HEAD_DIM
    qkv_piece = jnp.concatenate(
        [
            columns(w_query, lane * head_cols, head_cols),
            jnp.where(odd, columns(w_value, kv_at, HEAD_DIM), columns(w_key, kv_at, HEAD_DIM)),
        ],
        axis=1,
    )
    qkv_cols = head_cols + HEAD_DIM
    gain_rows = jnp.stack([attn_gain, mlp_gain]).astype(LOW)
    gain_reps = -(-own_width // qkv_cols)
    gain_rows = jnp.pad(gain_rows, ((0, 0), (0, gain_reps * qkv_cols - own_width)))
    gain_rows = gain_rows.reshape(2 * gain_reps, qkv_cols)
    gain_rows = jnp.pad(gain_rows, ((0, EXTRA - 2 * gain_reps), (0, 0)))
    qkv_parts = plane_parts(jnp.concatenate([qkv_piece, gain_rows], axis=0))
    qkv_mat = assemble([part[:own_width] for part in qkv_parts])
    gains = assemble(
        [
            part[own_width : own_width + 2 * gain_reps].reshape(2, -1)[:, :own_width]
            for part in qkv_parts
        ],
        1,
    )
    gain_one, gain_two = gains[0].astype(FULL), gains[1].astype(FULL)

    mlp_piece = jnp.concatenate(
        [
            columns(weight, p * ff_rows + lane * unit, unit)
            for weight in (w_gate, w_up)
            for p in range(planes)
        ],
        axis=1,
    )
    cut = (own_ff + 127) // 128 * 128
    first_piece = jnp.concatenate(
        [columns(w_out, lane * out_cols, out_cols), mlp_piece[:, :cut]], axis=1
    )
    second_piece = mlp_piece[:, cut:]
    first_piece, second_piece = lax.optimization_barrier((first_piece, second_piece))
    first_parts = plane_parts(first_piece)
    second_parts = plane_parts(second_piece)
    out_mat = assemble([part[:, :out_cols] for part in first_parts])
    mlp_mat = jnp.zeros((width, 2 * own_ff), LOW)
    for parts, start, place in ((first_parts, out_cols, 0), (second_parts, 0, cut)):
        for k, part in enumerate(parts):
            row = lax.rem(plane - k + planes, planes) * own_width
            mlp_mat = lax.dynamic_update_slice(mlp_mat, part[:, start:], (row, place))
    down_piece = lax.dynamic_slice_in_dim(w_down, lane * unit, unit, 0).astype(LOW)
    down_parts = plane_parts(down_piece)
    down_mat = assemble(down_parts)

    first_row = lane * head_cols
    owner = first_row // own_width
    row_piece = lax.dynamic_slice_in_dim(w_out, first_row - owner * own_width, head_cols, 0).astype(
        LOW
    )
    out_rows = jnp.where(owner == plane, row_piece, jnp.zeros_like(row_piece))
    for k in range(1, planes):
        pairs = []
        for d in range(lanes):
            source = (d * head_cols) // own_width
            pairs.append((d * planes + source, d * planes + (source + k) % planes))
        out_rows = out_rows + lax.ppermute(row_piece, ("dp", "shard"), pairs)

    grouped = table.reshape(seqs, planes, 2)
    order = lax.rem(plane - jnp.arange(planes, dtype=jnp.int32) + planes, planes)
    relative = jnp.take(grouped, order, axis=1)
    smaller = jnp.min(relative, axis=2)
    info = jnp.concatenate(
        [
            (relative[:, :, 0] > relative[:, :, 1]).astype(jnp.int32),
            (smaller < smaller[:, :1]).astype(jnp.int32),
        ],
        axis=1,
    )
    places = relative[:, 0, :, None] * span + jnp.arange(span, dtype=jnp.int32)
    frequency = ROPE_BASE ** (-(jnp.arange(HEAD_DIM // 2, dtype=FULL) * 2.0) / HEAD_DIM)
    angles = frequency[:, None] * places.reshape(-1).astype(FULL)[None, :]
    cosine, sine = jnp.cos(angles), jnp.sin(angles)

    wide = inputs.astype(FULL)
    scale_one = lax.rsqrt(jnp.mean(wide * wide, axis=-1, keepdims=True) + EPSILON)
    hidden_one = (wide * scale_one * gain_one).astype(LOW)
    qkv = contract(qkv_mat, hidden_one, 0, 1)
    half = qkv[head_cols:]
    half = jnp.where(odd, half, rope(half, cosine, sine)).astype(LOW)
    half_parts = plane_parts(half)
    query = rope(qkv[:head_cols].reshape(own_heads, HEAD_DIM, total_rows), cosine, sine)
    query = (query.astype(LOW).astype(FULL) * scale).astype(LOW).reshape(head_cols, total_rows)
    half_all = jnp.stack(half_parts, axis=0)
    other_half = swap_cores(half_all)
    key_all = jnp.where(odd, other_half, half_all)
    value_all = jnp.where(odd, half_all, other_half)
    attended, log_total = attn_forward(info, query, key_all, value_all, seqs)

    attended_all = lax.all_gather(attended, "dp", axis=0, tiled=True)
    branch = contract(out_mat, attended_all, 0, 0)
    own_inputs = lax.dynamic_slice_in_dim(inputs, lane * out_cols, out_cols, 1)
    middle_part = (own_inputs.astype(FULL).T + branch).astype(LOW)
    middle = lax.all_gather(middle_part, "dp", axis=0, tiled=True)
    wide_two = middle.astype(FULL)
    scale_two = lax.rsqrt(jnp.mean(wide_two * wide_two, axis=0, keepdims=True) + EPSILON)
    hidden_two = (wide_two * scale_two * gain_two[:, None]).astype(LOW)
    both = contract(mlp_mat, hidden_two, 0, 0)
    gate_value, up_value = both[:own_ff], both[own_ff:]
    sigmoid = jax.nn.sigmoid(gate_value)
    silu = gate_value * sigmoid
    inner = (silu * up_value).astype(LOW)

    inner_grad = contract(down_mat, upstream, 1, 1)
    gate_grad = inner_grad * up_value * sigmoid * (1.0 + gate_value * (1.0 - sigmoid))
    up_grad = inner_grad * silu
    both_grad = jnp.concatenate([gate_grad.astype(LOW), up_grad.astype(LOW)], axis=0)
    hidden_two_grad = contract(both_grad, mlp_mat, 0, 1).astype(LOW)
    hidden_two_own = lax.psum_scatter(hidden_two_grad, "dp", scatter_dimension=0, tiled=True)
    mlp_grad = contract(hidden_two, both_grad, 1, 1).astype(LOW)
    down_grad = contract(inner, upstream, 1, 0).astype(LOW)
    down_sent = plane_send(down_grad)
    mlp_sent = plane_send(mlp_grad)
    partial_out = contract(inner, down_mat, 0, 0).astype(LOW)
    hidden_two_own = hidden_two_own.astype(FULL)
    middle_own = lax.dynamic_slice_in_dim(middle, lane * rows, rows, 1).astype(FULL).T
    scale_own = lax.rsqrt(jnp.mean(middle_own * middle_own, axis=-1, keepdims=True) + EPSILON)
    normed_own = middle_own * scale_own
    gain_two_grad = jnp.sum(hidden_two_own * normed_own, axis=0)
    middle_grad = cotangent[0].astype(FULL) + norm_back(
        hidden_two_own, normed_own, scale_own, gain_two
    )
    middle_grad_low = middle_grad.astype(LOW)
    branch_grad = lax.all_gather(middle_grad_low, "dp", axis=0, tiled=True)

    partial_out, branch_grad = lax.optimization_barrier((partial_out, branch_grad))
    result = lax.psum_scatter(partial_out, "dp", scatter_dimension=0, tiled=True)
    block_out = (middle_own + result.astype(FULL)).astype(LOW)[None]

    attended_grad = contract(out_rows, branch_grad, 1, 1).astype(LOW)
    query_grad, key_grad, value_grad = attn_backward(
        info, query, key_all, value_all, attended, log_total, attended_grad, seqs
    )
    other_grad = swap_cores(jnp.where(odd, key_grad, value_grad))
    half_grad = (
        jnp.where(odd, value_grad, key_grad).astype(FULL) + other_grad.astype(FULL)
    ).astype(LOW)
    half_own = half_grad[0].astype(FULL)
    for k in range(1, planes):
        part = shift(half_grad[k], planes - k)
        half_own = half_own + part.astype(FULL)
    query_lin = rope(query_grad.reshape(own_heads, HEAD_DIM, total_rows), cosine, -sine)
    query_lin = query_lin.astype(LOW).reshape(head_cols, total_rows)
    half_lin = jnp.where(odd, half_own, rope(half_own, cosine, -sine)).astype(LOW)
    qkv_lin = jnp.concatenate([query_lin, half_lin], axis=0)
    hidden_one_part = contract(qkv_lin, qkv_mat, 0, 1)
    hidden_one_low = hidden_one_part.astype(LOW)
    hidden_one_grad = lax.psum_scatter(
        hidden_one_low, "dp", scatter_dimension=0, tiled=True
    ).astype(FULL)
    gain_one_grad = jnp.sum(hidden_one_low.astype(FULL) * (wide * scale_one), axis=0)
    own_tokens = tokens[0].astype(FULL)
    own_scale = lax.rsqrt(jnp.mean(own_tokens * own_tokens, axis=-1, keepdims=True) + EPSILON)
    input_norm_grad = norm_back(hidden_one_grad, own_tokens * own_scale, own_scale, gain_one)
    tokens_grad = (middle_grad + input_norm_grad)[None]

    branch_cols = lax.dynamic_slice_in_dim(branch_grad, lane * out_cols, out_cols, 1)
    qkv_grad = contract(hidden_one, qkv_lin, 0, 1).astype(LOW)
    out_grad = contract(attended_all, branch_cols, 1, 0).astype(LOW)
    piece_cols = qkv_cols + out_cols
    out_grad = lax.optimization_barrier(out_grad)
    attn_grad = jnp.concatenate([qkv_grad, out_grad], axis=1).reshape(planes, own_width, -1)
    gain_grads = jnp.stack([gain_one_grad, gain_two_grad]).astype(LOW)
    gain_grads = jnp.transpose(gain_grads.reshape(2, planes, own_width), (1, 0, 2))
    gain_grads = jnp.pad(gain_grads, ((0, 0), (0, EXTRA - 2), (0, piece_cols - own_width)))
    attn_grad = jnp.concatenate([attn_grad, gain_grads], axis=1)
    attn_sent = plane_send(attn_grad.reshape(-1, piece_cols))

    down_sum = plane_sum(down_sent)
    down_mine = jnp.stack(chip_stack(down_sum), axis=0)
    down_other = swap_cores(down_mine)
    mlp_sum = plane_sum(mlp_sent)
    mlp_mine = jnp.stack(chip_stack(mlp_sum), axis=0)
    mlp_other = swap_cores(mlp_mine)
    attn_sum = plane_sum(attn_sent)
    attn_mine = jnp.stack(chip_stack(attn_sum), axis=0)
    attn_other = swap_cores(attn_mine)

    lane_id = lane.astype(jnp.int32).reshape(1)
    if unit % 16 == 0:
        down_out = spread_down(lane_id, down_mine, down_other)
    else:
        down_out = lax.all_gather(down_sum, "dp", axis=0, tiled=True).astype(FULL)
    gate_out, up_out = spread_call(
        functools.partial(spread_mlp_kernel, lanes, planes, unit),
        lane_id,
        mlp_mine,
        mlp_other,
        own_width,
        min(64, own_width),
        (lanes * own_ff, lanes * own_ff),
    )
    query_out, key_out, value_out, out_out = spread_call(
        functools.partial(
            spread_attn_kernel, lanes, head_cols, out_cols, lanes // kv_heads
        ),
        lane_id,
        attn_mine,
        attn_other,
        own_width,
        EXTRA,
        (lanes * head_cols, kv_heads * HEAD_DIM, kv_heads * HEAD_DIM, lanes * out_cols),
    )
    gain_at = slice(own_width, own_width + 2)
    gain_own = jnp.sum(attn_mine[:, gain_at, :own_width].astype(FULL), axis=0) + jnp.sum(
        attn_other[:, gain_at, :own_width].astype(FULL), axis=0
    )
    return (
        block_out,
        tokens_grad,
        gain_own[0],
        query_out,
        key_out,
        value_out,
        out_out,
        gain_own[1],
        gate_out,
        up_out,
        down_out,
    )


def solution(mesh):
    rows = P("shard", None)
    acts = P("dp", "shard", None)
    gain = P("shard")
    weights = (gain, rows, rows, rows, rows, gain, rows, rows, rows)

    return jax.shard_map(
        on_device,
        mesh=mesh,
        in_specs=(acts, P("dp", None)) + weights + (acts,),
        out_specs=(acts, acts) + weights,
        check_vma=False,
    )
```

```python
import functools

import jax
import jax.numpy as jnp
from jax import lax
from jax.experimental import pallas as pl
from jax.experimental.pallas import tpu as pltpu
from jax.sharding import PartitionSpec as P

HEAD_DIM = 64
DP, SHARD = "dp", "shard"
EPSILON = 1e-05
ROPE_BASE = 10000.0
MASKED = -1e30
LOW = jnp.bfloat16
FULL = jnp.float32
EXTRA = 32


def contract(left, right, left_dim, right_dim):
    return lax.dot_general(
        left, right, (((left_dim,), (right_dim,)), ((), ())), preferred_element_type=FULL
    )


def shift(value, amount):
    count = lax.axis_size(SHARD)
    pairs = [(i, (i + amount) % count) for i in range(count)]
    return lax.ppermute(value, SHARD, pairs)


def swap_cores(value):
    lanes = lax.axis_size(DP)
    return lax.ppermute(value, DP, [(d, d ^ 1) for d in range(lanes)])


def swap_chips(value, mask):
    lanes = lax.axis_size(DP)
    return lax.ppermute(value, DP, [(d, d ^ (2 * mask)) for d in range(lanes)])


def plane_parts(value):
    count = lax.axis_size(SHARD)
    return [value] + [shift(value, k) for k in range(1, count)]


def assemble(parts, axis=0):
    count = lax.axis_size(SHARD)
    rank = lax.axis_index(SHARD)
    rows = parts[0].shape[axis]
    shape = list(parts[0].shape)
    shape[axis] = rows * count
    whole = jnp.zeros(shape, parts[0].dtype)
    for k, part in enumerate(parts):
        place = lax.rem(rank - k + count, count)
        whole = lax.dynamic_update_slice_in_dim(whole, part, place * rows, axis)
    return whole


def plane_send(value):
    count = lax.axis_size(SHARD)
    rank = lax.axis_index(SHARD)
    rows = value.shape[0] // count
    parts = []
    for k in range(count):
        target = lax.rem(rank + k, count)
        piece = lax.dynamic_slice_in_dim(value, target * rows, rows, 0)
        parts.append(shift(piece, k) if k else piece)
    return parts


def plane_sum(parts):
    total = parts[0].astype(FULL)
    for part in parts[1:]:
        total = total + part.astype(FULL)
    return total.astype(LOW)


def chip_stack(value):
    chips = lax.axis_size(DP) // 2
    return [value] + [swap_chips(value, k) for k in range(1, chips)]


def rope(values, cosine, sine):
    half = values.shape[-2] // 2
    front, back = values[..., :half, :], values[..., half:, :]
    return jnp.concatenate([front * cosine - back * sine, back * cosine + front * sine], axis=-2)


def norm_back(upstream, normed, row_scale, gain):
    scaled = upstream * gain
    mean = jnp.mean(scaled * normed, axis=-1, keepdims=True)
    return row_scale * (scaled - normed * mean)


class Tiles:
    def __init__(self, info_ref, planes, span, heads):
        self.info, self.planes, self.span, self.heads = info_ref, planes, span, heads
        self.seq = pl.program_id(0)

    def offset(self, part, high):
        first = self.info[self.seq, part]
        return pl.multiple_of(jnp.where(first == high, 0, 1) * self.span, self.span)

    def before(self, part):
        return self.info[self.seq, self.planes + part] == 1

    def picked(self, part, own):
        return jnp.where(self.before(part), self.offset(own, 0), self.offset(own, 1))

    def heads_of(self, ref, offset):
        offset = pl.multiple_of(offset, self.span)
        rows = [
            ref[h * HEAD_DIM : (h + 1) * HEAD_DIM, pl.ds(offset, self.span)]
            for h in range(self.heads)
        ]
        return jnp.concatenate(rows, axis=1)

    def put_heads(self, ref, offset, value):
        for h in range(self.heads):
            piece = value[:, h * self.span : (h + 1) * self.span]
            ref[h * HEAD_DIM : (h + 1) * HEAD_DIM, pl.ds(offset, self.span)] = piece.astype(
                ref.dtype
            )

    def block(self, ref, part, offset):
        return ref[part, :, pl.ds(pl.multiple_of(offset, self.span), self.span)]

    def diagonal(self):
        shape = (self.span, self.heads * self.span)
        keys = lax.broadcasted_iota(jnp.int32, shape, 0)
        queries = lax.broadcasted_iota(jnp.int32, shape, 1)
        return keys <= lax.rem(queries, self.span)


def top_of(value):
    return jnp.max(value, axis=0, keepdims=True)


def sum_of(value):
    return jnp.sum(value, axis=0, keepdims=True)


def attn_fwd_kernel(planes, span, heads, info_ref, q_ref, k_ref, v_ref, o_ref, lse_ref):
    tiles = Tiles(info_ref, planes, span, heads)
    low_at, high_at = tiles.offset(0, 0), tiles.offset(0, 1)
    q_low, q_high = tiles.heads_of(q_ref, low_at), tiles.heads_of(q_ref, high_at)
    visible = tiles.diagonal()

    def score(part, offset, query):
        return contract(tiles.block(k_ref, part, offset), query, 0, 0)

    own_low = jnp.where(visible, score(0, low_at, q_low), MASKED)
    own_high = jnp.where(visible, score(0, high_at, q_high), MASKED)
    wide = [score(p, tiles.offset(p, 0), q_high) for p in range(planes)]
    mixed = []
    for p in range(1, planes):
        query = tiles.heads_of(q_ref, tiles.picked(p, 0))
        mixed.append(score(p, tiles.picked(p, p), query))
    top_low, top_high = top_of(own_low), top_of(own_high)
    for value in wide:
        top_high = jnp.maximum(top_high, top_of(value))
    for p in range(1, planes):
        peak = top_of(mixed[p - 1])
        top_low = jnp.maximum(top_low, jnp.where(tiles.before(p), peak, MASKED))
        top_high = jnp.maximum(top_high, jnp.where(tiles.before(p), MASKED, peak))

    def add(part, offset, value, top):
        weight = jnp.exp(value - top)
        block = tiles.block(v_ref, part, offset)
        return sum_of(weight), contract(block, weight.astype(LOW), 1, 0)

    total_low, out_low = add(0, low_at, own_low, top_low)
    total_high, out_high = add(0, high_at, own_high, top_high)
    for p in range(planes):
        total, out = add(p, tiles.offset(p, 0), wide[p], top_high)
        total_high, out_high = total_high + total, out_high + out
    for p in range(1, planes):
        early = tiles.before(p)
        top = jnp.where(early, top_low, top_high)
        total, out = add(p, tiles.picked(p, p), mixed[p - 1], top)
        total_low = total_low + jnp.where(early, total, 0.0)
        total_high = total_high + jnp.where(early, 0.0, total)
        out_low = out_low + jnp.where(early, out, 0.0)
        out_high = out_high + jnp.where(early, 0.0, out)
    tiles.put_heads(o_ref, low_at, out_low / total_low)
    tiles.put_heads(o_ref, high_at, out_high / total_high)
    lse_ref[0, 0:1, :] = top_low + jnp.log(total_low)
    lse_ref[0, 1:2, :] = top_high + jnp.log(total_high)


def attn_bwd_kernel(
    planes, span, heads, info_ref, q_ref, k_ref, v_ref, o_ref, lse_ref, g_ref, dq_ref, dk_ref, dv_ref
):
    tiles = Tiles(info_ref, planes, span, heads)
    low_at, high_at = tiles.offset(0, 0), tiles.offset(0, 1)
    visible = tiles.diagonal()

    def state(offset, row):
        query, grad = tiles.heads_of(q_ref, offset), tiles.heads_of(g_ref, offset)
        out = tiles.heads_of(o_ref, offset)
        delta = sum_of(out.astype(FULL) * grad.astype(FULL))
        return query, grad, lse_ref[0, row : row + 1, :], delta

    low, high = state(low_at, 0), state(high_at, 1)

    def tile(part, offset, queries, masked=False):
        query, grad, log_total, delta = queries
        key, value = tiles.block(k_ref, part, offset), tiles.block(v_ref, part, offset)
        scores = contract(key, query, 0, 0)
        if masked:
            scores = jnp.where(visible, scores, MASKED)
        weight = jnp.exp(scores - log_total)
        change = contract(value, grad, 0, 0)
        change = (weight * (change - delta)).astype(LOW)
        dq = contract(key, change, 1, 0)
        dk = contract(query, change, 1, 1)
        dv = contract(grad, weight.astype(LOW), 1, 1)
        return dq, dk, dv

    dq_low, dk_low, dv_low = tile(0, low_at, low, True)
    dq_high, dk_high, dv_high = tile(0, high_at, high, True)

    def put(part, offset, dk, dv):
        place = pl.ds(pl.multiple_of(offset, span), span)
        dk_ref[part, :, place] = dk.astype(dk_ref.dtype)
        dv_ref[part, :, place] = dv.astype(dv_ref.dtype)

    put(0, high_at, dk_high, dv_high)
    for p in range(planes):
        dq, dk, dv = tile(p, tiles.offset(p, 0), high)
        dq_high = dq_high + dq
        if p == 0:
            put(0, low_at, dk_low + dk, dv_low + dv)
            continue
        early = tiles.before(p)
        at = tiles.picked(p, 0)
        queries = (
            tiles.heads_of(q_ref, at),
            tiles.heads_of(g_ref, at),
            jnp.where(early, low[2], high[2]),
            jnp.where(early, low[3], high[3]),
        )
        dq, dk_mixed, dv_mixed = tile(p, tiles.picked(p, p), queries)
        dq_low = dq_low + jnp.where(early, dq, 0.0)
        dq_high = dq_high + jnp.where(early, 0.0, dq)
        put(
            p,
            tiles.offset(p, 0),
            dk + jnp.where(early, dk_mixed, 0.0),
            dv + jnp.where(early, dv_mixed, 0.0),
        )
        put(
            p,
            tiles.offset(p, 1),
            jnp.where(early, 0.0, dk_mixed),
            jnp.where(early, 0.0, dv_mixed),
        )
    scale = HEAD_DIM ** (-0.5)
    tiles.put_heads(dq_ref, low_at, dq_low * scale)
    tiles.put_heads(dq_ref, high_at, dq_high * scale)


def attn_specs(planes, rows, cols, heads):
    act = pl.BlockSpec((cols, rows), lambda s, info: (0, s))
    keys = pl.BlockSpec((planes, HEAD_DIM, rows), lambda s, info: (0, 0, s))
    lse = pl.BlockSpec((1, 2, heads * rows // 2), lambda s, info: (s, 0, 0))
    return act, keys, lse


def attn_cost(seqs, planes, rows, cols, dots):
    pairs = seqs * rows * rows // 4 * (2 * planes + 1) * (cols // HEAD_DIM)
    return pl.CostEstimate(
        flops=2 * dots * pairs * HEAD_DIM,
        bytes_accessed=2 * seqs * rows * (3 * cols + 4 * planes * HEAD_DIM),
        transcendentals=pairs,
    )


def attn_forward(info, query, key, value, seqs):
    planes, cols = key.shape[0], query.shape[0]
    rows, heads = query.shape[1] // seqs, cols // HEAD_DIM
    act, keys, lse = attn_specs(planes, rows, cols, heads)
    return pl.pallas_call(
        functools.partial(attn_fwd_kernel, planes, rows // 2, heads),
        out_shape=(
            jax.ShapeDtypeStruct(query.shape, LOW),
            jax.ShapeDtypeStruct((seqs, 2, heads * rows // 2), FULL),
        ),
        grid_spec=pltpu.PrefetchScalarGridSpec(
            num_scalar_prefetch=1,
            grid=(seqs,),
            in_specs=[act, keys, keys],
            out_specs=(act, lse),
        ),
        cost_estimate=attn_cost(seqs, planes, rows, cols, 2),
    )(info, query, key, value)


def attn_backward(info, query, key, value, out, lse_value, grad, seqs):
    planes, cols = key.shape[0], query.shape[0]
    rows, heads = query.shape[1] // seqs, cols // HEAD_DIM
    act, keys, lse = attn_specs(planes, rows, cols, heads)
    return pl.pallas_call(
        functools.partial(attn_bwd_kernel, planes, rows // 2, heads),
        out_shape=(
            jax.ShapeDtypeStruct(query.shape, FULL),
            jax.ShapeDtypeStruct(key.shape, LOW),
            jax.ShapeDtypeStruct(key.shape, LOW),
        ),
        grid_spec=pltpu.PrefetchScalarGridSpec(
            num_scalar_prefetch=1,
            grid=(seqs,),
            in_specs=[act, keys, keys, act, lse, act],
            out_specs=(act, keys, keys),
        ),
        cost_estimate=attn_cost(seqs, planes, rows, cols, 5),
    )(info, query, key, value, out, lse_value, grad)


def picker(lane_ref, mine_ref, other_ref):
    lane = lane_ref[0]
    chip, core = lane // 2, lane % 2

    def pick(d, *index):
        slot = (d // 2) ^ chip
        mine = mine_ref[(slot,) + index].astype(FULL)
        other = other_ref[(slot,) + index].astype(FULL)
        return jnp.where(core == d % 2, mine, other)

    return pick


def spread_mlp_kernel(lanes, planes, unit, lane_ref, mine_ref, other_ref, gate_ref, up_ref):
    pick = picker(lane_ref, mine_ref, other_ref)
    every = slice(None)
    for which, out_ref in enumerate((gate_ref, up_ref)):
        for p in range(planes):
            for d in range(lanes):
                start = (which * planes + p) * unit
                place = (p * lanes + d) * unit
                out_ref[:, place : place + unit] = pick(d, every, slice(start, start + unit))


def spread_attn_kernel(
    lanes, head_cols, out_cols, sharing, lane_ref, mine_ref, other_ref, q_ref, k_ref, v_ref, o_ref
):
    pick = picker(lane_ref, mine_ref, other_ref)
    every = slice(None)
    middle = head_cols + HEAD_DIM
    for d in range(lanes):
        q_ref[:, d * head_cols : (d + 1) * head_cols] = pick(d, every, slice(0, head_cols))
        o_ref[:, d * out_cols : (d + 1) * out_cols] = pick(
            d, every, slice(middle, middle + out_cols)
        )
    for h in range(lanes // sharing):
        for first, out_ref in ((0, k_ref), (1, v_ref)):
            total = None
            for d in range(h * sharing + first, (h + 1) * sharing, 2):
                part = pick(d, every, slice(head_cols, middle))
                total = part if total is None else total + part
            out_ref[:, h * HEAD_DIM : (h + 1) * HEAD_DIM] = total


def spread_down_kernel(lane_ref, mine_ref, other_ref, out_ref):
    core = lane_ref[0] % 2
    mine, other = mine_ref[0].astype(FULL), other_ref[0].astype(FULL)
    out_ref[...] = jnp.where(core == pl.program_id(0) % 2, mine, other)


def spread_call(kernel, lane, mine, other, rows, block, widths):
    chips, _, cols = mine.shape
    spec = pl.BlockSpec((chips, block, cols), lambda i, lane_ref: (0, i, 0))
    return pl.pallas_call(
        kernel,
        out_shape=tuple(jax.ShapeDtypeStruct((rows, w), FULL) for w in widths),
        grid_spec=pltpu.PrefetchScalarGridSpec(
            num_scalar_prefetch=1,
            grid=(rows // block,),
            in_specs=[spec, spec],
            out_specs=tuple(pl.BlockSpec((block, w), lambda i, lane_ref: (i, 0)) for w in widths),
        ),
        cost_estimate=pl.CostEstimate(
            flops=0, bytes_accessed=chips * rows * cols * 12, transcendentals=0
        ),
    )(lane, mine, other)


def spread_down(lane, mine, other):
    chips, rows, cols = mine.shape
    spec = pl.BlockSpec(
        (1, rows, cols), lambda d, lane_ref: ((d // 2) ^ (lane_ref[0] // 2), 0, 0)
    )
    return pl.pallas_call(
        spread_down_kernel,
        out_shape=jax.ShapeDtypeStruct((2 * chips * rows, cols), FULL),
        grid_spec=pltpu.PrefetchScalarGridSpec(
            num_scalar_prefetch=1,
            grid=(2 * chips,),
            in_specs=[spec, spec],
            out_specs=pl.BlockSpec((rows, cols), lambda d, lane_ref: (d, 0)),
        ),
        cost_estimate=pl.CostEstimate(
            flops=0, bytes_accessed=chips * rows * cols * 12, transcendentals=0
        ),
    )(lane, mine, other)


def on_device(
    tokens,
    block_order,
    attn_gain,
    w_query,
    w_key,
    w_value,
    w_out,
    mlp_gain,
    w_gate,
    w_up,
    w_down,
    cotangent,
):
    planes = lax.axis_size(SHARD)
    plane = lax.axis_index(SHARD)
    lanes = lax.axis_size(DP)
    lane = lax.axis_index(DP)
    odd = lax.rem(lane, 2) == 1
    rows = tokens.shape[1]
    width = tokens.shape[2]
    span = rows // 2
    seqs = lanes
    total_rows = seqs * rows
    own_width = width // planes
    heads = w_query.shape[1] // HEAD_DIM
    kv_heads = w_key.shape[1] // HEAD_DIM
    own_heads = heads // lanes
    head_cols = own_heads * HEAD_DIM
    kv_head = (lane * own_heads * kv_heads) // heads
    out_cols = w_out.shape[1] // lanes
    ff_rows = w_down.shape[0]
    unit = ff_rows // lanes
    own_ff = unit * planes
    scale = HEAD_DIM ** (-0.5)

    inputs = lax.all_gather(tokens[0], DP, axis=0, tiled=True)
    upstream = lax.all_gather(cotangent[0], DP, axis=0, tiled=True)
    table = lax.all_gather(block_order[0], DP, axis=0, tiled=False)

    def columns(weight, start, count):
        return lax.dynamic_slice_in_dim(weight, start, count, 1).astype(LOW)

    kv_at = kv_head * HEAD_DIM
    qkv_piece = jnp.concatenate(
        [
            columns(w_query, lane * head_cols, head_cols),
            jnp.where(odd, columns(w_value, kv_at, HEAD_DIM), columns(w_key, kv_at, HEAD_DIM)),
        ],
        axis=1,
    )
    qkv_cols = head_cols + HEAD_DIM
    gain_rows = jnp.stack([attn_gain, mlp_gain]).astype(LOW)
    gain_reps = -(-own_width // qkv_cols)
    gain_rows = jnp.pad(gain_rows, ((0, 0), (0, gain_reps * qkv_cols - own_width)))
    gain_rows = gain_rows.reshape(2 * gain_reps, qkv_cols)
    gain_rows = jnp.pad(gain_rows, ((0, EXTRA - 2 * gain_reps), (0, 0)))
    qkv_parts = plane_parts(jnp.concatenate([qkv_piece, gain_rows], axis=0))
    qkv_mat = assemble([part[:own_width] for part in qkv_parts])
    gains = assemble(
        [
            part[own_width : own_width + 2 * gain_reps].reshape(2, -1)[:, :own_width]
            for part in qkv_parts
        ],
        1,
    )
    gain_one, gain_two = gains[0].astype(FULL), gains[1].astype(FULL)

    mlp_piece = jnp.concatenate(
        [
            columns(weight, p * ff_rows + lane * unit, unit)
            for weight in (w_gate, w_up)
            for p in range(planes)
        ],
        axis=1,
    )
    cut = 128
    first_piece = jnp.concatenate(
        [columns(w_out, lane * out_cols, out_cols), mlp_piece[:, :cut]], axis=1
    )
    second_piece = mlp_piece[:, cut:]
    first_piece, second_piece = lax.optimization_barrier((first_piece, second_piece))
    first_parts = plane_parts(first_piece)
    second_parts = plane_parts(second_piece)
    out_mat = assemble([part[:, :out_cols] for part in first_parts])
    mlp_mat = jnp.zeros((width, 2 * own_ff), LOW)
    for parts, start, place in ((first_parts, out_cols, 0), (second_parts, 0, cut)):
        for k, part in enumerate(parts):
            row = lax.rem(plane - k + planes, planes) * own_width
            mlp_mat = lax.dynamic_update_slice(mlp_mat, part[:, start:], (row, place))
    down_piece = lax.dynamic_slice_in_dim(w_down, lane * unit, unit, 0).astype(LOW)
    down_parts = plane_parts(down_piece)
    down_mat = assemble(down_parts)

    grouped = table.reshape(seqs, planes, 2)
    order = lax.rem(plane - jnp.arange(planes, dtype=jnp.int32) + planes, planes)
    relative = jnp.take(grouped, order, axis=1)
    smaller = jnp.min(relative, axis=2)
    info = jnp.concatenate(
        [
            (relative[:, :, 0] > relative[:, :, 1]).astype(jnp.int32),
            (smaller < smaller[:, :1]).astype(jnp.int32),
        ],
        axis=1,
    )
    places = relative[:, 0, :, None] * span + jnp.arange(span, dtype=jnp.int32)
    frequency = ROPE_BASE ** (-(jnp.arange(HEAD_DIM // 2, dtype=FULL) * 2.0) / HEAD_DIM)
    angles = frequency[:, None] * places.reshape(-1).astype(FULL)[None, :]
    cosine, sine = jnp.cos(angles), jnp.sin(angles)

    wide = inputs.astype(FULL)
    scale_one = lax.rsqrt(jnp.mean(wide * wide, axis=-1, keepdims=True) + EPSILON)
    hidden_one = (wide * scale_one * gain_one).astype(LOW)
    qkv = contract(qkv_mat, hidden_one, 0, 1)
    half = qkv[head_cols:]
    half = jnp.where(odd, half, rope(half, cosine, sine)).astype(LOW)
    half_parts = plane_parts(half)
    query = rope(qkv[:head_cols].reshape(own_heads, HEAD_DIM, total_rows), cosine, sine)
    query = (query.astype(LOW).astype(FULL) * scale).astype(LOW).reshape(head_cols, total_rows)
    half_all = jnp.stack(half_parts, axis=0)
    other_half = swap_cores(half_all)
    key_all = jnp.where(odd, other_half, half_all)
    value_all = jnp.where(odd, half_all, other_half)
    attended, log_total = attn_forward(info, query, key_all, value_all, seqs)

    attended_all = lax.all_gather(attended, DP, axis=0, tiled=True)
    branch = contract(out_mat, attended_all, 0, 0)
    own_inputs = lax.dynamic_slice_in_dim(inputs, lane * out_cols, out_cols, 1)
    out_rows = jnp.zeros((head_cols, lanes * out_cols), LOW)
    for m in range(lanes):
        peer = lane ^ m
        block = lax.dynamic_slice_in_dim(out_mat, peer * head_cols, head_cols, 0)
        if m:
            block = lax.ppermute(block, DP, [(d, d ^ m) for d in range(lanes)])
        out_rows = lax.dynamic_update_slice_in_dim(out_rows, block, peer * out_cols, 1)
    middle_part = (own_inputs.astype(FULL).T + branch).astype(LOW)
    middle = lax.all_gather(middle_part, DP, axis=0, tiled=True)
    wide_two = middle.astype(FULL)
    scale_two = lax.rsqrt(jnp.mean(wide_two * wide_two, axis=0, keepdims=True) + EPSILON)
    hidden_two = (wide_two * scale_two * gain_two[:, None]).astype(LOW)
    both = contract(mlp_mat, hidden_two, 0, 0)
    gate_value, up_value = both[:own_ff], both[own_ff:]
    sigmoid = jax.nn.sigmoid(gate_value)
    silu = gate_value * sigmoid
    inner = (silu * up_value).astype(LOW)

    inner_grad = contract(down_mat, upstream, 1, 1)
    gate_grad = inner_grad * up_value * sigmoid * (1.0 + gate_value * (1.0 - sigmoid))
    up_grad = inner_grad * silu
    both_grad = jnp.concatenate([gate_grad.astype(LOW), up_grad.astype(LOW)], axis=0)
    hidden_two_grad = contract(both_grad, mlp_mat, 0, 1).astype(LOW)
    hidden_two_own = lax.psum_scatter(hidden_two_grad, DP, scatter_dimension=0, tiled=True)
    mlp_grad = contract(hidden_two, both_grad, 1, 1).astype(LOW)
    down_grad = contract(inner, upstream, 1, 0).astype(LOW)
    down_sent = plane_send(down_grad)
    tail = own_width * 3 // 16
    mlp_grad = mlp_grad.reshape(planes, own_width, 2 * own_ff)
    mlp_sent = plane_send(mlp_grad[:, :-tail].reshape(-1, 2 * own_ff))
    mlp_tail_sent = plane_send(mlp_grad[:, -tail:].reshape(-1, 2 * own_ff))
    partial_out = contract(inner, down_mat, 0, 0).astype(LOW)
    hidden_two_own = hidden_two_own.astype(FULL)
    middle_own = lax.dynamic_slice_in_dim(middle, lane * rows, rows, 1).astype(FULL).T
    scale_own = lax.rsqrt(jnp.mean(middle_own * middle_own, axis=-1, keepdims=True) + EPSILON)
    normed_own = middle_own * scale_own
    gain_two_grad = jnp.sum(hidden_two_own * normed_own, axis=0)
    middle_grad = cotangent[0].astype(FULL) + norm_back(
        hidden_two_own, normed_own, scale_own, gain_two
    )
    middle_grad_low = middle_grad.astype(LOW)
    branch_grad = lax.all_gather(middle_grad_low, DP, axis=0, tiled=True)

    partial_out, branch_grad = lax.optimization_barrier((partial_out, branch_grad))
    result = lax.psum_scatter(partial_out, DP, scatter_dimension=0, tiled=True)
    block_out = (middle_own + result.astype(FULL)).astype(LOW)[None]

    attended_grad = contract(out_rows, branch_grad, 1, 1).astype(LOW)
    query_grad, key_grad, value_grad = attn_backward(
        info, query, key_all, value_all, attended, log_total, attended_grad, seqs
    )
    other_grad = swap_cores(jnp.where(odd, key_grad, value_grad))
    half_grad = (
        jnp.where(odd, value_grad, key_grad).astype(FULL) + other_grad.astype(FULL)
    ).astype(LOW)
    half_own = half_grad[0].astype(FULL)
    for k in range(1, planes):
        part = shift(half_grad[k], planes - k)
        half_own = half_own + part.astype(FULL)
    query_lin = rope(query_grad.reshape(own_heads, HEAD_DIM, total_rows), cosine, -sine)
    query_lin = query_lin.astype(LOW).reshape(head_cols, total_rows)
    half_lin = jnp.where(odd, half_own, rope(half_own, cosine, -sine)).astype(LOW)
    qkv_lin = jnp.concatenate([query_lin, half_lin], axis=0)
    hidden_one_part = contract(qkv_lin, qkv_mat, 0, 1)
    hidden_one_low = hidden_one_part.astype(LOW)
    hidden_one_grad = lax.psum_scatter(
        hidden_one_low, DP, scatter_dimension=0, tiled=True
    ).astype(FULL)
    gain_one_grad = jnp.sum(hidden_one_low.astype(FULL) * (wide * scale_one), axis=0)
    own_tokens = tokens[0].astype(FULL)
    own_scale = lax.rsqrt(jnp.mean(own_tokens * own_tokens, axis=-1, keepdims=True) + EPSILON)
    input_norm_grad = norm_back(hidden_one_grad, own_tokens * own_scale, own_scale, gain_one)
    tokens_grad = (middle_grad + input_norm_grad)[None]

    branch_cols = lax.dynamic_slice_in_dim(branch_grad, lane * out_cols, out_cols, 1)
    qkv_grad = contract(hidden_one, qkv_lin, 0, 1).astype(LOW)
    out_grad = contract(attended_all, branch_cols, 1, 0).astype(LOW)
    piece_cols = qkv_cols + out_cols
    out_grad = lax.optimization_barrier(out_grad)
    attn_grad = jnp.concatenate([qkv_grad, out_grad], axis=1).reshape(planes, own_width, -1)
    gain_grads = jnp.stack([gain_one_grad, gain_two_grad]).astype(LOW)
    gain_grads = jnp.transpose(gain_grads.reshape(2, planes, own_width), (1, 0, 2))
    gain_grads = jnp.pad(gain_grads, ((0, 0), (0, EXTRA - 2), (0, piece_cols - own_width)))
    attn_grad = jnp.concatenate([attn_grad, gain_grads], axis=1)
    attn_sent = plane_send(attn_grad.reshape(-1, piece_cols))

    down_sum = plane_sum(down_sent)
    down_mine = jnp.stack(chip_stack(down_sum), axis=0)
    down_other = swap_cores(down_mine)
    mlp_sum = jnp.concatenate([plane_sum(mlp_sent), plane_sum(mlp_tail_sent)], axis=0)
    mlp_mine = jnp.stack(chip_stack(mlp_sum), axis=0)
    mlp_other = swap_cores(mlp_mine)
    attn_sum = plane_sum(attn_sent)
    attn_mine = jnp.stack(chip_stack(attn_sum), axis=0)
    attn_other = swap_cores(attn_mine)

    lane_id = lane.astype(jnp.int32).reshape(1)
    if unit % 16 == 0:
        down_out = spread_down(lane_id, down_mine, down_other)
    else:
        down_out = lax.all_gather(down_sum, DP, axis=0, tiled=True).astype(FULL)
    gate_out, up_out = spread_call(
        functools.partial(spread_mlp_kernel, lanes, planes, unit),
        lane_id,
        mlp_mine,
        mlp_other,
        own_width,
        min(64, own_width),
        (lanes * own_ff, lanes * own_ff),
    )
    query_out, key_out, value_out, out_out = spread_call(
        functools.partial(
            spread_attn_kernel, lanes, head_cols, out_cols, lanes // kv_heads
        ),
        lane_id,
        attn_mine,
        attn_other,
        own_width,
        EXTRA,
        (lanes * head_cols, kv_heads * HEAD_DIM, kv_heads * HEAD_DIM, lanes * out_cols),
    )
    gain_at = slice(own_width, own_width + 2)
    gain_own = jnp.sum(attn_mine[:, gain_at, :own_width].astype(FULL), axis=0) + jnp.sum(
        attn_other[:, gain_at, :own_width].astype(FULL), axis=0
    )
    return (
        block_out,
        tokens_grad,
        gain_own[0],
        query_out,
        key_out,
        value_out,
        out_out,
        gain_own[1],
        gate_out,
        up_out,
        down_out,
    )


def solution(mesh):
    rows = P(SHARD, None)
    acts = P(DP, SHARD, None)
    gain = P(SHARD)
    weights = (gain, rows, rows, rows, rows, gain, rows, rows, rows)

    return jax.shard_map(
        on_device,
        mesh=mesh,
        in_specs=(acts, P(DP, None)) + weights + (acts,),
        out_specs=(acts, acts) + weights,
        check_vma=False,
    )
```

```python
import functools

import jax
import jax.numpy as jnp
from jax import lax
from jax.experimental import pallas as pl
from jax.experimental.pallas import tpu as pltpu
from jax.sharding import PartitionSpec as P

HEAD_DIM = 64
DP, SHARD = "dp", "shard"
EPSILON = 1e-05
ROPE_BASE = 10000.0
MASKED = -1e30
LOW = jnp.bfloat16
FULL = jnp.float32
EXTRA = 32


def contract(left, right, left_dim, right_dim):
    return lax.dot_general(
        left, right, (((left_dim,), (right_dim,)), ((), ())), preferred_element_type=FULL
    )


def shift(value, amount):
    count = lax.axis_size(SHARD)
    pairs = [(i, (i + amount) % count) for i in range(count)]
    return lax.ppermute(value, SHARD, pairs)


def swap_cores(value):
    lanes = lax.axis_size(DP)
    return lax.ppermute(value, DP, [(d, d ^ 1) for d in range(lanes)])


def swap_chips(value, mask):
    lanes = lax.axis_size(DP)
    pairs = [(d, d ^ (2 * mask)) for d in range(lanes)]
    return lax.ppermute(value, DP, pairs)


def plane_parts(value):
    count = lax.axis_size(SHARD)
    return [value] + [shift(value, k) for k in range(1, count)]


def placed(parts):
    count = lax.axis_size(SHARD)
    rank = lax.axis_index(SHARD)
    return [(part, lax.rem(rank - k + count, count)) for k, part in enumerate(parts)]


def forwarded(value):
    count = lax.axis_size(SHARD)
    rank = lax.axis_index(SHARD)
    if count != 4:
        return placed(plane_parts(value))
    across = shift(value, 2)
    up = lax.ppermute(value, SHARD, [(0, 1), (1, 2), (2, 3)])
    down = lax.ppermute(value, SHARD, [(1, 0), (2, 1), (3, 2)])
    far = lax.ppermute(across, SHARD, [(2, 3), (1, 0)])
    edge = (rank == 0) | (rank == 3)
    far_place = jnp.where(edge, 3 - rank, rank)
    return [
        (value, rank),
        (up, lax.rem(rank + 3, 4)),
        (down, lax.rem(rank + 1, 4)),
        (across, lax.rem(rank + 2, 4)),
        (jnp.where(edge, far, value), far_place),
    ]


def assemble(pieces, axis=0):
    count = lax.axis_size(SHARD)
    rows = pieces[0][0].shape[axis]
    shape = list(pieces[0][0].shape)
    shape[axis] = rows * count
    whole = jnp.zeros(shape, pieces[0][0].dtype)
    for part, place in pieces:
        whole = lax.dynamic_update_slice_in_dim(whole, part, place * rows, axis)
    return whole


def plane_send(value):
    count = lax.axis_size(SHARD)
    rank = lax.axis_index(SHARD)
    rows = value.shape[0] // count
    parts = []
    for k in range(count):
        target = lax.rem(rank + k, count)
        piece = lax.dynamic_slice_in_dim(value, target * rows, rows, 0)
        parts.append(shift(piece, k) if k else piece)
    return parts


def plane_sum(parts):
    total = parts[0].astype(FULL)
    for part in parts[1:]:
        total = total + part.astype(FULL)
    return total.astype(LOW)


def chip_stack(value):
    chips = lax.axis_size(DP) // 2
    return [value] + [swap_chips(value, k) for k in range(1, chips)]


def rope(values, cosine, sine):
    half = values.shape[-2] // 2
    front, back = values[..., :half, :], values[..., half:, :]
    return jnp.concatenate([front * cosine - back * sine, back * cosine + front * sine], axis=-2)


def norm_back(upstream, normed, row_scale, gain):
    scaled = upstream * gain
    mean = jnp.mean(scaled * normed, axis=-1, keepdims=True)
    return row_scale * (scaled - normed * mean)


class Tiles:
    def __init__(self, info_ref, planes, span, heads):
        self.info, self.planes, self.span, self.heads = info_ref, planes, span, heads
        self.seq = pl.program_id(0)

    def offset(self, part, high):
        first = self.info[self.seq, part]
        return pl.multiple_of(jnp.where(first == high, 0, 1) * self.span, self.span)

    def before(self, part):
        return self.info[self.seq, self.planes + part] == 1

    def picked(self, part, own):
        return jnp.where(self.before(part), self.offset(own, 0), self.offset(own, 1))

    def heads_of(self, ref, offset):
        offset = pl.multiple_of(offset, self.span)
        rows = [
            ref[h * HEAD_DIM : (h + 1) * HEAD_DIM, pl.ds(offset, self.span)]
            for h in range(self.heads)
        ]
        return jnp.concatenate(rows, axis=1)

    def put_heads(self, ref, offset, value):
        for h in range(self.heads):
            piece = value[:, h * self.span : (h + 1) * self.span]
            ref[h * HEAD_DIM : (h + 1) * HEAD_DIM, pl.ds(offset, self.span)] = piece.astype(
                ref.dtype
            )

    def block(self, ref, part, offset):
        return ref[part, :, pl.ds(pl.multiple_of(offset, self.span), self.span)]

    def diagonal(self):
        shape = (self.span, self.heads * self.span)
        keys = lax.broadcasted_iota(jnp.int32, shape, 0)
        queries = lax.broadcasted_iota(jnp.int32, shape, 1)
        return keys <= lax.rem(queries, self.span)


def top_of(value):
    return jnp.max(value, axis=0, keepdims=True)


def sum_of(value):
    return jnp.sum(value, axis=0, keepdims=True)


def attn_fwd_kernel(planes, span, heads, info_ref, q_ref, k_ref, v_ref, o_ref, lse_ref):
    tiles = Tiles(info_ref, planes, span, heads)
    low_at, high_at = tiles.offset(0, 0), tiles.offset(0, 1)
    q_low, q_high = tiles.heads_of(q_ref, low_at), tiles.heads_of(q_ref, high_at)
    visible = tiles.diagonal()

    def score(part, offset, query):
        return contract(tiles.block(k_ref, part, offset), query, 0, 0)

    own_low = jnp.where(visible, score(0, low_at, q_low), MASKED)
    own_high = jnp.where(visible, score(0, high_at, q_high), MASKED)
    wide = [score(p, tiles.offset(p, 0), q_high) for p in range(planes)]
    mixed = []
    for p in range(1, planes):
        query = tiles.heads_of(q_ref, tiles.picked(p, 0))
        mixed.append(score(p, tiles.picked(p, p), query))
    top_low, top_high = top_of(own_low), top_of(own_high)
    for value in wide:
        top_high = jnp.maximum(top_high, top_of(value))
    for p in range(1, planes):
        peak = top_of(mixed[p - 1])
        top_low = jnp.maximum(top_low, jnp.where(tiles.before(p), peak, MASKED))
        top_high = jnp.maximum(top_high, jnp.where(tiles.before(p), MASKED, peak))

    def add(part, offset, value, top):
        weight = jnp.exp(value - top)
        block = tiles.block(v_ref, part, offset)
        return sum_of(weight), contract(block, weight.astype(LOW), 1, 0)

    total_low, out_low = add(0, low_at, own_low, top_low)
    total_high, out_high = add(0, high_at, own_high, top_high)
    for p in range(planes):
        total, out = add(p, tiles.offset(p, 0), wide[p], top_high)
        total_high, out_high = total_high + total, out_high + out
    for p in range(1, planes):
        early = tiles.before(p)
        top = jnp.where(early, top_low, top_high)
        total, out = add(p, tiles.picked(p, p), mixed[p - 1], top)
        total_low = total_low + jnp.where(early, total, 0.0)
        total_high = total_high + jnp.where(early, 0.0, total)
        out_low = out_low + jnp.where(early, out, 0.0)
        out_high = out_high + jnp.where(early, 0.0, out)
    tiles.put_heads(o_ref, low_at, out_low / total_low)
    tiles.put_heads(o_ref, high_at, out_high / total_high)
    lse_ref[0, 0:1, :] = top_low + jnp.log(total_low)
    lse_ref[0, 1:2, :] = top_high + jnp.log(total_high)


def attn_bwd_kernel(
    planes, span, heads, info_ref, q_ref, k_ref, v_ref, o_ref, lse_ref, g_ref, dq_ref, dk_ref, dv_ref
):
    tiles = Tiles(info_ref, planes, span, heads)
    low_at, high_at = tiles.offset(0, 0), tiles.offset(0, 1)
    visible = tiles.diagonal()

    def state(offset, row):
        query, grad = tiles.heads_of(q_ref, offset), tiles.heads_of(g_ref, offset)
        out = tiles.heads_of(o_ref, offset)
        delta = sum_of(out.astype(FULL) * grad.astype(FULL))
        return query, grad, lse_ref[0, row : row + 1, :], delta

    low, high = state(low_at, 0), state(high_at, 1)

    def tile(part, offset, queries, masked=False):
        query, grad, log_total, delta = queries
        key, value = tiles.block(k_ref, part, offset), tiles.block(v_ref, part, offset)
        scores = contract(key, query, 0, 0)
        if masked:
            scores = jnp.where(visible, scores, MASKED)
        weight = jnp.exp(scores - log_total)
        change = contract(value, grad, 0, 0)
        change = (weight * (change - delta)).astype(LOW)
        dq = contract(key, change, 1, 0)
        dk = contract(query, change, 1, 1)
        dv = contract(grad, weight.astype(LOW), 1, 1)
        return dq, dk, dv

    dq_low, dk_low, dv_low = tile(0, low_at, low, True)
    dq_high, dk_high, dv_high = tile(0, high_at, high, True)

    def put(part, offset, dk, dv):
        place = pl.ds(pl.multiple_of(offset, span), span)
        dk_ref[part, :, place] = dk.astype(dk_ref.dtype)
        dv_ref[part, :, place] = dv.astype(dv_ref.dtype)

    put(0, high_at, dk_high, dv_high)
    for p in range(planes):
        dq, dk, dv = tile(p, tiles.offset(p, 0), high)
        dq_high = dq_high + dq
        if p == 0:
            put(0, low_at, dk_low + dk, dv_low + dv)
            continue
        early = tiles.before(p)
        at = tiles.picked(p, 0)
        queries = (
            tiles.heads_of(q_ref, at),
            tiles.heads_of(g_ref, at),
            jnp.where(early, low[2], high[2]),
            jnp.where(early, low[3], high[3]),
        )
        dq, dk_mixed, dv_mixed = tile(p, tiles.picked(p, p), queries)
        dq_low = dq_low + jnp.where(early, dq, 0.0)
        dq_high = dq_high + jnp.where(early, 0.0, dq)
        put(
            p,
            tiles.offset(p, 0),
            dk + jnp.where(early, dk_mixed, 0.0),
            dv + jnp.where(early, dv_mixed, 0.0),
        )
        put(
            p,
            tiles.offset(p, 1),
            jnp.where(early, 0.0, dk_mixed),
            jnp.where(early, 0.0, dv_mixed),
        )
    scale = HEAD_DIM ** (-0.5)
    tiles.put_heads(dq_ref, low_at, dq_low * scale)
    tiles.put_heads(dq_ref, high_at, dq_high * scale)


def attn_specs(planes, rows, cols, heads):
    act = pl.BlockSpec((cols, rows), lambda s, info: (0, s))
    keys = pl.BlockSpec((planes, HEAD_DIM, rows), lambda s, info: (0, 0, s))
    lse = pl.BlockSpec((1, 2, heads * rows // 2), lambda s, info: (s, 0, 0))
    return act, keys, lse


def attn_cost(seqs, planes, rows, cols, dots):
    pairs = seqs * rows * rows // 4 * (2 * planes + 1) * (cols // HEAD_DIM)
    return pl.CostEstimate(
        flops=2 * dots * pairs * HEAD_DIM,
        bytes_accessed=2 * seqs * rows * (3 * cols + 4 * planes * HEAD_DIM),
        transcendentals=pairs,
    )


def attn_forward(info, query, key, value, seqs):
    planes, cols = key.shape[0], query.shape[0]
    rows, heads = query.shape[1] // seqs, cols // HEAD_DIM
    act, keys, lse = attn_specs(planes, rows, cols, heads)
    return pl.pallas_call(
        functools.partial(attn_fwd_kernel, planes, rows // 2, heads),
        out_shape=(
            jax.ShapeDtypeStruct(query.shape, LOW),
            jax.ShapeDtypeStruct((seqs, 2, heads * rows // 2), FULL),
        ),
        grid_spec=pltpu.PrefetchScalarGridSpec(
            num_scalar_prefetch=1,
            grid=(seqs,),
            in_specs=[act, keys, keys],
            out_specs=(act, lse),
        ),
        cost_estimate=attn_cost(seqs, planes, rows, cols, 2),
    )(info, query, key, value)


def attn_backward(info, query, key, value, out, lse_value, grad, seqs):
    planes, cols = key.shape[0], query.shape[0]
    rows, heads = query.shape[1] // seqs, cols // HEAD_DIM
    act, keys, lse = attn_specs(planes, rows, cols, heads)
    return pl.pallas_call(
        functools.partial(attn_bwd_kernel, planes, rows // 2, heads),
        out_shape=(
            jax.ShapeDtypeStruct(query.shape, FULL),
            jax.ShapeDtypeStruct(key.shape, LOW),
            jax.ShapeDtypeStruct(key.shape, LOW),
        ),
        grid_spec=pltpu.PrefetchScalarGridSpec(
            num_scalar_prefetch=1,
            grid=(seqs,),
            in_specs=[act, keys, keys, act, lse, act],
            out_specs=(act, keys, keys),
        ),
        cost_estimate=attn_cost(seqs, planes, rows, cols, 5),
    )(info, query, key, value, out, lse_value, grad)


def picker(lane_ref, mine_ref, other_ref):
    lane = lane_ref[0]
    chip, core = lane // 2, lane % 2

    def pick(d, *index):
        slot = (d // 2) ^ chip
        mine = mine_ref[(slot,) + index].astype(FULL)
        other = other_ref[(slot,) + index].astype(FULL)
        return jnp.where(core == d % 2, mine, other)

    return pick


def spread_mlp_kernel(lanes, planes, unit, lane_ref, mine_ref, other_ref, gate_ref, up_ref):
    pick = picker(lane_ref, mine_ref, other_ref)
    every = slice(None)
    for which, out_ref in enumerate((gate_ref, up_ref)):
        for p in range(planes):
            for d in range(lanes):
                start = (which * planes + p) * unit
                place = (p * lanes + d) * unit
                out_ref[:, place : place + unit] = pick(d, every, slice(start, start + unit))


def spread_attn_kernel(
    lanes, head_cols, out_cols, sharing, lane_ref, mine_ref, other_ref, q_ref, k_ref, v_ref, o_ref
):
    pick = picker(lane_ref, mine_ref, other_ref)
    every = slice(None)
    middle = head_cols + HEAD_DIM
    for d in range(lanes):
        q_ref[:, d * head_cols : (d + 1) * head_cols] = pick(d, every, slice(0, head_cols))
        o_ref[:, d * out_cols : (d + 1) * out_cols] = pick(
            d, every, slice(middle, middle + out_cols)
        )
    for h in range(lanes // sharing):
        for first, out_ref in ((0, k_ref), (1, v_ref)):
            total = None
            for d in range(h * sharing + first, (h + 1) * sharing, 2):
                part = pick(d, every, slice(head_cols, middle))
                total = part if total is None else total + part
            out_ref[:, h * HEAD_DIM : (h + 1) * HEAD_DIM] = total


def spread_down_kernel(lane_ref, mine_ref, other_ref, out_ref):
    core = lane_ref[0] % 2
    mine, other = mine_ref[0].astype(FULL), other_ref[0].astype(FULL)
    out_ref[...] = jnp.where(core == pl.program_id(0) % 2, mine, other)


def spread_call(kernel, lane, mine, other, rows, block, widths):
    chips, _, cols = mine.shape
    spec = pl.BlockSpec((chips, block, cols), lambda i, lane_ref: (0, i, 0))
    return pl.pallas_call(
        kernel,
        out_shape=tuple(jax.ShapeDtypeStruct((rows, w), FULL) for w in widths),
        grid_spec=pltpu.PrefetchScalarGridSpec(
            num_scalar_prefetch=1,
            grid=(rows // block,),
            in_specs=[spec, spec],
            out_specs=tuple(pl.BlockSpec((block, w), lambda i, lane_ref: (i, 0)) for w in widths),
        ),
        cost_estimate=pl.CostEstimate(
            flops=0, bytes_accessed=chips * rows * cols * 12, transcendentals=0
        ),
    )(lane, mine, other)


def spread_down(lane, mine, other):
    chips, rows, cols = mine.shape
    spec = pl.BlockSpec(
        (1, rows, cols), lambda d, lane_ref: ((d // 2) ^ (lane_ref[0] // 2), 0, 0)
    )
    return pl.pallas_call(
        spread_down_kernel,
        out_shape=jax.ShapeDtypeStruct((2 * chips * rows, cols), FULL),
        grid_spec=pltpu.PrefetchScalarGridSpec(
            num_scalar_prefetch=1,
            grid=(2 * chips,),
            in_specs=[spec, spec],
            out_specs=pl.BlockSpec((rows, cols), lambda d, lane_ref: (d, 0)),
        ),
        cost_estimate=pl.CostEstimate(
            flops=0, bytes_accessed=chips * rows * cols * 12, transcendentals=0
        ),
    )(lane, mine, other)


def on_device(
    tokens,
    block_order,
    attn_gain,
    w_query,
    w_key,
    w_value,
    w_out,
    mlp_gain,
    w_gate,
    w_up,
    w_down,
    cotangent,
):
    planes = lax.axis_size(SHARD)
    plane = lax.axis_index(SHARD)
    lanes = lax.axis_size(DP)
    lane = lax.axis_index(DP)
    odd = lax.rem(lane, 2) == 1
    rows = tokens.shape[1]
    width = tokens.shape[2]
    span = rows // 2
    seqs = lanes
    total_rows = seqs * rows
    own_width = width // planes
    heads = w_query.shape[1] // HEAD_DIM
    kv_heads = w_key.shape[1] // HEAD_DIM
    own_heads = heads // lanes
    head_cols = own_heads * HEAD_DIM
    kv_head = (lane * own_heads * kv_heads) // heads
    out_cols = w_out.shape[1] // lanes
    ff_rows = w_down.shape[0]
    unit = ff_rows // lanes
    own_ff = unit * planes
    scale = HEAD_DIM ** (-0.5)

    inputs = lax.all_gather(tokens[0], DP, axis=0, tiled=True)
    upstream = lax.all_gather(cotangent[0], DP, axis=0, tiled=True)
    table = lax.all_gather(block_order[0], DP, axis=0, tiled=False)

    def columns(weight, start, count):
        return lax.dynamic_slice_in_dim(weight, start, count, 1).astype(LOW)

    kv_at = kv_head * HEAD_DIM
    qkv_piece = jnp.concatenate(
        [
            columns(w_query, lane * head_cols, head_cols),
            jnp.where(odd, columns(w_value, kv_at, HEAD_DIM), columns(w_key, kv_at, HEAD_DIM)),
        ],
        axis=1,
    )
    qkv_cols = head_cols + HEAD_DIM
    gain_rows = jnp.stack([attn_gain, mlp_gain]).astype(LOW)
    gain_reps = -(-own_width // qkv_cols)
    gain_rows = jnp.pad(gain_rows, ((0, 0), (0, gain_reps * qkv_cols - own_width)))
    gain_rows = gain_rows.reshape(2 * gain_reps, qkv_cols)
    gain_rows = jnp.pad(gain_rows, ((0, EXTRA - 2 * gain_reps), (0, 0)))
    qkv_parts = plane_parts(jnp.concatenate([qkv_piece, gain_rows], axis=0))
    qkv_mat = assemble(placed([part[:own_width] for part in qkv_parts]))
    gain_parts = [
        part[own_width : own_width + 2 * gain_reps].reshape(2, -1)[:, :own_width]
        for part in qkv_parts
    ]
    gains = assemble(placed(gain_parts), 1)
    gain_one, gain_two = gains[0].astype(FULL), gains[1].astype(FULL)

    mlp_piece = jnp.concatenate(
        [
            columns(weight, p * ff_rows + lane * unit, unit)
            for weight in (w_gate, w_up)
            for p in range(planes)
        ],
        axis=1,
    )
    cut = 128
    first_piece = jnp.concatenate(
        [columns(w_out, lane * out_cols, out_cols), mlp_piece[:, :cut]], axis=1
    )
    second_piece = mlp_piece[:, cut:]
    first_piece, second_piece = lax.optimization_barrier((first_piece, second_piece))
    first_parts = plane_parts(first_piece)
    second_pieces = forwarded(second_piece)
    out_mat = assemble(placed([part[:, :out_cols] for part in first_parts]))
    mlp_mat = jnp.zeros((width, 2 * own_ff), LOW)
    for part, place in placed([part[:, out_cols:] for part in first_parts]):
        mlp_mat = lax.dynamic_update_slice(mlp_mat, part, (place * own_width, 0))
    for part, place in second_pieces[:-1]:
        mlp_mat = lax.dynamic_update_slice(mlp_mat, part, (place * own_width, cut))
    part, place = second_pieces[-1]
    mlp_mat = lax.dynamic_update_slice(mlp_mat, part, (place * own_width, cut))
    down_piece = lax.dynamic_slice_in_dim(w_down, lane * unit, unit, 0).astype(LOW)
    down_mat = assemble(forwarded(down_piece))

    grouped = table.reshape(seqs, planes, 2)
    order = lax.rem(plane - jnp.arange(planes, dtype=jnp.int32) + planes, planes)
    relative = jnp.take(grouped, order, axis=1)
    smaller = jnp.min(relative, axis=2)
    info = jnp.concatenate(
        [
            (relative[:, :, 0] > relative[:, :, 1]).astype(jnp.int32),
            (smaller < smaller[:, :1]).astype(jnp.int32),
        ],
        axis=1,
    )
    places = relative[:, 0, :, None] * span + jnp.arange(span, dtype=jnp.int32)
    frequency = ROPE_BASE ** (-(jnp.arange(HEAD_DIM // 2, dtype=FULL) * 2.0) / HEAD_DIM)
    angles = frequency[:, None] * places.reshape(-1).astype(FULL)[None, :]
    cosine, sine = jnp.cos(angles), jnp.sin(angles)

    wide = inputs.astype(FULL)
    scale_one = lax.rsqrt(jnp.mean(wide * wide, axis=-1, keepdims=True) + EPSILON)
    hidden_one = (wide * scale_one * gain_one).astype(LOW)
    qkv = contract(qkv_mat, hidden_one, 0, 1)
    half = qkv[head_cols:]
    half = jnp.where(odd, half, rope(half, cosine, sine)).astype(LOW)
    half_parts = plane_parts(half)
    query = rope(qkv[:head_cols].reshape(own_heads, HEAD_DIM, total_rows), cosine, sine)
    query = (query.astype(LOW).astype(FULL) * scale).astype(LOW).reshape(head_cols, total_rows)
    half_all = jnp.stack(half_parts, axis=0)
    other_half = swap_cores(half_all)
    key_all = jnp.where(odd, other_half, half_all)
    value_all = jnp.where(odd, half_all, other_half)
    attended, log_total = attn_forward(info, query, key_all, value_all, seqs)

    attended_all = lax.all_gather(attended, DP, axis=0, tiled=True)
    branch = contract(out_mat, attended_all, 0, 0)
    own_inputs = lax.dynamic_slice_in_dim(inputs, lane * out_cols, out_cols, 1)
    out_rows = jnp.zeros((head_cols, lanes * out_cols), LOW)
    for m in range(lanes):
        peer = lane ^ m
        block = lax.dynamic_slice_in_dim(out_mat, peer * head_cols, head_cols, 0)
        if m:
            block = lax.ppermute(block, DP, [(d, d ^ m) for d in range(lanes)])
        out_rows = lax.dynamic_update_slice_in_dim(out_rows, block, peer * out_cols, 1)
    middle_part = (own_inputs.astype(FULL).T + branch).astype(LOW)
    middle = lax.all_gather(middle_part, DP, axis=0, tiled=True)
    wide_two = middle.astype(FULL)
    scale_two = lax.rsqrt(jnp.mean(wide_two * wide_two, axis=0, keepdims=True) + EPSILON)
    hidden_two = (wide_two * scale_two * gain_two[:, None]).astype(LOW)
    both = contract(mlp_mat, hidden_two, 0, 0)
    gate_value, up_value = both[:own_ff], both[own_ff:]
    sigmoid = jax.nn.sigmoid(gate_value)
    silu = gate_value * sigmoid
    inner = (silu * up_value).astype(LOW)

    inner_grad = contract(down_mat, upstream, 1, 1)
    gate_grad = inner_grad * up_value * sigmoid * (1.0 + gate_value * (1.0 - sigmoid))
    up_grad = inner_grad * silu
    both_grad = jnp.concatenate([gate_grad.astype(LOW), up_grad.astype(LOW)], axis=0)
    hidden_two_grad = contract(both_grad, mlp_mat, 0, 1).astype(LOW)
    hidden_two_own = lax.psum_scatter(hidden_two_grad, DP, scatter_dimension=0, tiled=True)
    mlp_grad = contract(hidden_two, both_grad, 1, 1).astype(LOW)
    down_grad = contract(inner, upstream, 1, 0).astype(LOW)
    down_sent = plane_send(down_grad)
    tail = own_width * 3 // 16
    mlp_grad = mlp_grad.reshape(planes, own_width, 2 * own_ff)
    mlp_sent = plane_send(mlp_grad[:, :-tail].reshape(-1, 2 * own_ff))
    mlp_tail_sent = plane_send(mlp_grad[:, -tail:].reshape(-1, 2 * own_ff))
    partial_out = contract(inner, down_mat, 0, 0).astype(LOW)
    hidden_two_own = hidden_two_own.astype(FULL)
    middle_own = lax.dynamic_slice_in_dim(middle, lane * rows, rows, 1).astype(FULL).T
    scale_own = lax.rsqrt(jnp.mean(middle_own * middle_own, axis=-1, keepdims=True) + EPSILON)
    normed_own = middle_own * scale_own
    gain_two_grad = jnp.sum(hidden_two_own * normed_own, axis=0)
    middle_grad = cotangent[0].astype(FULL) + norm_back(
        hidden_two_own, normed_own, scale_own, gain_two
    )
    middle_grad_low = middle_grad.astype(LOW)
    branch_grad = lax.all_gather(middle_grad_low, DP, axis=0, tiled=True)

    partial_out, branch_grad = lax.optimization_barrier((partial_out, branch_grad))
    result = lax.psum_scatter(partial_out, DP, scatter_dimension=0, tiled=True)
    block_out = (middle_own + result.astype(FULL)).astype(LOW)[None]

    attended_grad = contract(out_rows, branch_grad, 1, 1).astype(LOW)
    query_grad, key_grad, value_grad = attn_backward(
        info, query, key_all, value_all, attended, log_total, attended_grad, seqs
    )
    other_grad = swap_cores(jnp.where(odd, key_grad, value_grad))
    half_grad = (
        jnp.where(odd, value_grad, key_grad).astype(FULL) + other_grad.astype(FULL)
    ).astype(LOW)
    half_own = half_grad[0].astype(FULL)
    for k in range(1, planes):
        part = shift(half_grad[k], planes - k)
        half_own = half_own + part.astype(FULL)
    query_lin = rope(query_grad.reshape(own_heads, HEAD_DIM, total_rows), cosine, -sine)
    query_lin = query_lin.astype(LOW).reshape(head_cols, total_rows)
    half_lin = jnp.where(odd, half_own, rope(half_own, cosine, -sine)).astype(LOW)
    qkv_lin = jnp.concatenate([query_lin, half_lin], axis=0)
    hidden_one_part = contract(qkv_lin, qkv_mat, 0, 1)
    hidden_one_low = hidden_one_part.astype(LOW)
    hidden_one_grad = lax.psum_scatter(
        hidden_one_low, DP, scatter_dimension=0, tiled=True
    ).astype(FULL)
    gain_one_grad = jnp.sum(hidden_one_low.astype(FULL) * (wide * scale_one), axis=0)
    own_tokens = tokens[0].astype(FULL)
    own_scale = lax.rsqrt(jnp.mean(own_tokens * own_tokens, axis=-1, keepdims=True) + EPSILON)
    input_norm_grad = norm_back(hidden_one_grad, own_tokens * own_scale, own_scale, gain_one)
    tokens_grad = (middle_grad + input_norm_grad)[None]

    branch_cols = lax.dynamic_slice_in_dim(branch_grad, lane * out_cols, out_cols, 1)
    qkv_grad = contract(hidden_one, qkv_lin, 0, 1).astype(LOW)
    out_grad = contract(attended_all, branch_cols, 1, 0).astype(LOW)
    out_grad = lax.optimization_barrier(out_grad)
    attn_grad = jnp.concatenate([qkv_grad, out_grad], axis=1).reshape(planes, own_width, -1)
    attn_grad = jnp.pad(attn_grad, ((0, 0), (0, 16), (0, 0)))
    attn_sent = plane_send(attn_grad.reshape(planes * (own_width + 16), -1))
    gain_grads = jnp.stack([gain_one_grad, gain_two_grad])
    gain_grads = jnp.transpose(gain_grads.reshape(2, planes, own_width), (1, 0, 2))
    gain_sent = plane_send(gain_grads.reshape(2 * planes, own_width))
    gain_own = sum(gain_sent[1:], gain_sent[0])
    gain_stack = chip_stack(gain_own)
    gain_own = sum(gain_stack[1:], gain_stack[0])
    gain_own = gain_own + swap_cores(gain_own)

    down_sum = plane_sum(down_sent)
    down_mine = jnp.stack(chip_stack(down_sum), axis=0)
    down_other = swap_cores(down_mine)
    mlp_sum = jnp.concatenate([plane_sum(mlp_sent), plane_sum(mlp_tail_sent)], axis=0)
    mlp_mine = jnp.stack(chip_stack(mlp_sum), axis=0)
    mlp_other = swap_cores(mlp_mine)
    attn_sum = plane_sum(attn_sent)
    attn_mine = jnp.stack(chip_stack(attn_sum), axis=0)
    attn_other = swap_cores(attn_mine)

    lane_id = lane.astype(jnp.int32).reshape(1)
    if unit % 16 == 0:
        down_out = spread_down(lane_id, down_mine, down_other)
    else:
        down_out = lax.all_gather(down_sum, DP, axis=0, tiled=True).astype(FULL)
    gate_out, up_out = spread_call(
        functools.partial(spread_mlp_kernel, lanes, planes, unit),
        lane_id,
        mlp_mine,
        mlp_other,
        own_width,
        min(64, own_width),
        (lanes * own_ff, lanes * own_ff),
    )
    query_out, key_out, value_out, out_out = spread_call(
        functools.partial(
            spread_attn_kernel, lanes, head_cols, out_cols, lanes // kv_heads
        ),
        lane_id,
        attn_mine,
        attn_other,
        own_width,
        EXTRA,
        (lanes * head_cols, kv_heads * HEAD_DIM, kv_heads * HEAD_DIM, lanes * out_cols),
    )
    return (
        block_out,
        tokens_grad,
        gain_own[0],
        query_out,
        key_out,
        value_out,
        out_out,
        gain_own[1],
        gate_out,
        up_out,
        down_out,
    )


def solution(mesh):
    rows = P(SHARD, None)
    acts = P(DP, SHARD, None)
    gain = P(SHARD)
    weights = (gain, rows, rows, rows, rows, gain, rows, rows, rows)

    return jax.shard_map(
        on_device,
        mesh=mesh,
        in_specs=(acts, P(DP, None)) + weights + (acts,),
        out_specs=(acts, acts) + weights,
        check_vma=False,
    )
```

```python
import functools

import jax
import jax.numpy as jnp
from jax import lax
from jax.experimental import pallas as pl
from jax.experimental.pallas import tpu as pltpu
from jax.sharding import PartitionSpec as P

HEAD_DIM = 64
DP, SHARD = "dp", "shard"
EPSILON = 1e-05
ROPE_BASE = 10000.0
MASKED = -1e30
LOW = jnp.bfloat16
FULL = jnp.float32
EXTRA = 32


def contract(left, right, left_dim, right_dim):
    return lax.dot_general(
        left, right, (((left_dim,), (right_dim,)), ((), ())), preferred_element_type=FULL
    )


def shift(value, amount):
    count = lax.axis_size(SHARD)
    pairs = [(i, (i + amount) % count) for i in range(count)]
    return lax.ppermute(value, SHARD, pairs)


def swap_cores(value):
    lanes = lax.axis_size(DP)
    return lax.ppermute(value, DP, [(d, d ^ 1) for d in range(lanes)])


def swap_chips(value, mask):
    lanes = lax.axis_size(DP)
    pairs = [(d, d ^ (2 * mask)) for d in range(lanes)]
    return lax.ppermute(value, DP, pairs)


def plane_parts(value):
    count = lax.axis_size(SHARD)
    return [value] + [shift(value, k) for k in range(1, count)]


def placed(parts):
    count = lax.axis_size(SHARD)
    rank = lax.axis_index(SHARD)
    return [(part, lax.rem(rank - k + count, count)) for k, part in enumerate(parts)]


def forwarded(value):
    count = lax.axis_size(SHARD)
    rank = lax.axis_index(SHARD)
    if count != 4:
        return placed(plane_parts(value))
    across = shift(value, 2)
    up = lax.ppermute(value, SHARD, [(0, 1), (1, 2), (2, 3)])
    down = lax.ppermute(value, SHARD, [(1, 0), (2, 1), (3, 2)])
    far = lax.ppermute(across, SHARD, [(2, 3), (1, 0)])
    edge = (rank == 0) | (rank == 3)
    far_place = jnp.where(edge, 3 - rank, rank)
    return [
        (value, rank),
        (up, lax.rem(rank + 3, 4)),
        (down, lax.rem(rank + 1, 4)),
        (across, lax.rem(rank + 2, 4)),
        (jnp.where(edge, far, value), far_place),
    ]


def assemble(pieces, axis=0):
    count = lax.axis_size(SHARD)
    rows = pieces[0][0].shape[axis]
    shape = list(pieces[0][0].shape)
    shape[axis] = rows * count
    whole = jnp.zeros(shape, pieces[0][0].dtype)
    for part, place in pieces:
        whole = lax.dynamic_update_slice_in_dim(whole, part, place * rows, axis)
    return whole


def plane_send(value):
    count = lax.axis_size(SHARD)
    rank = lax.axis_index(SHARD)
    rows = value.shape[0] // count
    parts = []
    for k in range(count):
        target = lax.rem(rank + k, count)
        piece = lax.dynamic_slice_in_dim(value, target * rows, rows, 0)
        parts.append(shift(piece, k) if k else piece)
    return parts


def plane_sum(parts):
    total = parts[0].astype(FULL)
    for part in parts[1:]:
        total = total + part.astype(FULL)
    return total.astype(LOW)


def chip_stack(value):
    chips = lax.axis_size(DP) // 2
    return [value] + [swap_chips(value, k) for k in range(1, chips)]


def rope(values, cosine, sine):
    half = values.shape[-2] // 2
    front, back = values[..., :half, :], values[..., half:, :]
    return jnp.concatenate([front * cosine - back * sine, back * cosine + front * sine], axis=-2)


def norm_back(upstream, normed, row_scale, gain):
    scaled = upstream * gain
    mean = jnp.mean(scaled * normed, axis=-1, keepdims=True)
    return row_scale * (scaled - normed * mean)


class Tiles:
    def __init__(self, info_ref, planes, span, heads):
        self.info, self.planes, self.span, self.heads = info_ref, planes, span, heads
        self.seq = pl.program_id(0)

    def offset(self, part, high):
        first = self.info[self.seq, part]
        return pl.multiple_of(jnp.where(first == high, 0, 1) * self.span, self.span)

    def before(self, part):
        return self.info[self.seq, self.planes + part] == 1

    def picked(self, part, own):
        return jnp.where(self.before(part), self.offset(own, 0), self.offset(own, 1))

    def heads_of(self, ref, offset):
        offset = pl.multiple_of(offset, self.span)
        rows = [
            ref[h * HEAD_DIM : (h + 1) * HEAD_DIM, pl.ds(offset, self.span)]
            for h in range(self.heads)
        ]
        return jnp.concatenate(rows, axis=1)

    def put_heads(self, ref, offset, value):
        for h in range(self.heads):
            piece = value[:, h * self.span : (h + 1) * self.span]
            ref[h * HEAD_DIM : (h + 1) * HEAD_DIM, pl.ds(offset, self.span)] = piece.astype(
                ref.dtype
            )

    def block(self, ref, part, offset):
        return ref[part, :, pl.ds(pl.multiple_of(offset, self.span), self.span)]

    def diagonal(self):
        shape = (self.span, self.heads * self.span)
        keys = lax.broadcasted_iota(jnp.int32, shape, 0)
        queries = lax.broadcasted_iota(jnp.int32, shape, 1)
        return keys <= lax.rem(queries, self.span)


def top_of(value):
    return jnp.max(value, axis=0, keepdims=True)


def sum_of(value):
    return jnp.sum(value, axis=0, keepdims=True)


def attn_fwd_kernel(planes, span, heads, info_ref, q_ref, k_ref, v_ref, o_ref, lse_ref):
    tiles = Tiles(info_ref, planes, span, heads)
    low_at, high_at = tiles.offset(0, 0), tiles.offset(0, 1)
    q_low, q_high = tiles.heads_of(q_ref, low_at), tiles.heads_of(q_ref, high_at)
    visible = tiles.diagonal()

    def score(part, offset, query):
        return contract(tiles.block(k_ref, part, offset), query, 0, 0)

    own_low = jnp.where(visible, score(0, low_at, q_low), MASKED)
    own_high = jnp.where(visible, score(0, high_at, q_high), MASKED)
    wide = [score(p, tiles.offset(p, 0), q_high) for p in range(planes)]
    mixed = []
    for p in range(1, planes):
        query = tiles.heads_of(q_ref, tiles.picked(p, 0))
        mixed.append(score(p, tiles.picked(p, p), query))
    top_low, top_high = top_of(own_low), top_of(own_high)
    for value in wide:
        top_high = jnp.maximum(top_high, top_of(value))
    for p in range(1, planes):
        peak = top_of(mixed[p - 1])
        top_low = jnp.maximum(top_low, jnp.where(tiles.before(p), peak, MASKED))
        top_high = jnp.maximum(top_high, jnp.where(tiles.before(p), MASKED, peak))

    def add(part, offset, value, top):
        weight = jnp.exp(value - top)
        block = tiles.block(v_ref, part, offset)
        return sum_of(weight), contract(block, weight.astype(LOW), 1, 0)

    total_low, out_low = add(0, low_at, own_low, top_low)
    total_high, out_high = add(0, high_at, own_high, top_high)
    for p in range(planes):
        total, out = add(p, tiles.offset(p, 0), wide[p], top_high)
        total_high, out_high = total_high + total, out_high + out
    for p in range(1, planes):
        early = tiles.before(p)
        top = jnp.where(early, top_low, top_high)
        total, out = add(p, tiles.picked(p, p), mixed[p - 1], top)
        total_low = total_low + jnp.where(early, total, 0.0)
        total_high = total_high + jnp.where(early, 0.0, total)
        out_low = out_low + jnp.where(early, out, 0.0)
        out_high = out_high + jnp.where(early, 0.0, out)
    tiles.put_heads(o_ref, low_at, out_low / total_low)
    tiles.put_heads(o_ref, high_at, out_high / total_high)
    lse_ref[0, 0:1, :] = top_low + jnp.log(total_low)
    lse_ref[0, 1:2, :] = top_high + jnp.log(total_high)


def attn_bwd_kernel(
    planes, span, heads, info_ref, q_ref, k_ref, v_ref, o_ref, lse_ref, g_ref, dq_ref, dk_ref, dv_ref
):
    tiles = Tiles(info_ref, planes, span, heads)
    low_at, high_at = tiles.offset(0, 0), tiles.offset(0, 1)
    visible = tiles.diagonal()

    def state(offset, row):
        query, grad = tiles.heads_of(q_ref, offset), tiles.heads_of(g_ref, offset)
        out = tiles.heads_of(o_ref, offset)
        delta = sum_of(out.astype(FULL) * grad.astype(FULL))
        return query, grad, lse_ref[0, row : row + 1, :], delta

    low, high = state(low_at, 0), state(high_at, 1)

    def tile(part, offset, queries, masked=False):
        query, grad, log_total, delta = queries
        key, value = tiles.block(k_ref, part, offset), tiles.block(v_ref, part, offset)
        scores = contract(key, query, 0, 0)
        if masked:
            scores = jnp.where(visible, scores, MASKED)
        weight = jnp.exp(scores - log_total)
        change = contract(value, grad, 0, 0)
        change = (weight * (change - delta)).astype(LOW)
        dq = contract(key, change, 1, 0)
        dk = contract(query, change, 1, 1)
        dv = contract(grad, weight.astype(LOW), 1, 1)
        return dq, dk, dv

    dq_low, dk_low, dv_low = tile(0, low_at, low, True)
    dq_high, dk_high, dv_high = tile(0, high_at, high, True)

    def put(part, offset, dk, dv):
        place = pl.ds(pl.multiple_of(offset, span), span)
        dk_ref[part, :, place] = dk.astype(dk_ref.dtype)
        dv_ref[part, :, place] = dv.astype(dv_ref.dtype)

    put(0, high_at, dk_high, dv_high)
    for p in range(planes):
        dq, dk, dv = tile(p, tiles.offset(p, 0), high)
        dq_high = dq_high + dq
        if p == 0:
            put(0, low_at, dk_low + dk, dv_low + dv)
            continue
        early = tiles.before(p)
        at = tiles.picked(p, 0)
        queries = (
            tiles.heads_of(q_ref, at),
            tiles.heads_of(g_ref, at),
            jnp.where(early, low[2], high[2]),
            jnp.where(early, low[3], high[3]),
        )
        dq, dk_mixed, dv_mixed = tile(p, tiles.picked(p, p), queries)
        dq_low = dq_low + jnp.where(early, dq, 0.0)
        dq_high = dq_high + jnp.where(early, 0.0, dq)
        put(
            p,
            tiles.offset(p, 0),
            dk + jnp.where(early, dk_mixed, 0.0),
            dv + jnp.where(early, dv_mixed, 0.0),
        )
        put(
            p,
            tiles.offset(p, 1),
            jnp.where(early, 0.0, dk_mixed),
            jnp.where(early, 0.0, dv_mixed),
        )
    scale = HEAD_DIM ** (-0.5)
    tiles.put_heads(dq_ref, low_at, dq_low * scale)
    tiles.put_heads(dq_ref, high_at, dq_high * scale)


def attn_specs(planes, rows, cols, heads):
    act = pl.BlockSpec((cols, rows), lambda s, info: (0, s))
    keys = pl.BlockSpec((planes, HEAD_DIM, rows), lambda s, info: (0, 0, s))
    lse = pl.BlockSpec((1, 2, heads * rows // 2), lambda s, info: (s, 0, 0))
    return act, keys, lse


def attn_cost(seqs, planes, rows, cols, dots):
    pairs = seqs * rows * rows // 4 * (2 * planes + 1) * (cols // HEAD_DIM)
    return pl.CostEstimate(
        flops=2 * dots * pairs * HEAD_DIM,
        bytes_accessed=2 * seqs * rows * (3 * cols + 4 * planes * HEAD_DIM),
        transcendentals=pairs,
    )


def attn_forward(info, query, key, value, seqs):
    planes, cols = key.shape[0], query.shape[0]
    rows, heads = query.shape[1] // seqs, cols // HEAD_DIM
    act, keys, lse = attn_specs(planes, rows, cols, heads)
    return pl.pallas_call(
        functools.partial(attn_fwd_kernel, planes, rows // 2, heads),
        out_shape=(
            jax.ShapeDtypeStruct(query.shape, LOW),
            jax.ShapeDtypeStruct((seqs, 2, heads * rows // 2), FULL),
        ),
        grid_spec=pltpu.PrefetchScalarGridSpec(
            num_scalar_prefetch=1,
            grid=(seqs,),
            in_specs=[act, keys, keys],
            out_specs=(act, lse),
        ),
        cost_estimate=attn_cost(seqs, planes, rows, cols, 2),
    )(info, query, key, value)


def attn_backward(info, query, key, value, out, lse_value, grad, seqs):
    planes, cols = key.shape[0], query.shape[0]
    rows, heads = query.shape[1] // seqs, cols // HEAD_DIM
    act, keys, lse = attn_specs(planes, rows, cols, heads)
    return pl.pallas_call(
        functools.partial(attn_bwd_kernel, planes, rows // 2, heads),
        out_shape=(
            jax.ShapeDtypeStruct(query.shape, FULL),
            jax.ShapeDtypeStruct(key.shape, LOW),
            jax.ShapeDtypeStruct(key.shape, LOW),
        ),
        grid_spec=pltpu.PrefetchScalarGridSpec(
            num_scalar_prefetch=1,
            grid=(seqs,),
            in_specs=[act, keys, keys, act, lse, act],
            out_specs=(act, keys, keys),
        ),
        cost_estimate=attn_cost(seqs, planes, rows, cols, 5),
    )(info, query, key, value, out, lse_value, grad)


def picker(lane_ref, mine_ref, other_ref):
    lane = lane_ref[0]
    chip, core = lane // 2, lane % 2

    def pick(d, *index):
        slot = (d // 2) ^ chip
        mine = mine_ref[(slot,) + index].astype(FULL)
        other = other_ref[(slot,) + index].astype(FULL)
        return jnp.where(core == d % 2, mine, other)

    return pick


def spread_mlp_kernel(lanes, planes, unit, lane_ref, mine_ref, other_ref, gate_ref, up_ref):
    pick = picker(lane_ref, mine_ref, other_ref)
    every = slice(None)
    for which, out_ref in enumerate((gate_ref, up_ref)):
        for p in range(planes):
            for d in range(lanes):
                start = (which * planes + p) * unit
                place = (p * lanes + d) * unit
                out_ref[:, place : place + unit] = pick(d, every, slice(start, start + unit))


def spread_attn_kernel(
    lanes, head_cols, out_cols, sharing, lane_ref, mine_ref, other_ref, q_ref, k_ref, v_ref, o_ref
):
    pick = picker(lane_ref, mine_ref, other_ref)
    every = slice(None)
    middle = head_cols + HEAD_DIM
    for d in range(lanes):
        q_ref[:, d * head_cols : (d + 1) * head_cols] = pick(d, every, slice(0, head_cols))
        o_ref[:, d * out_cols : (d + 1) * out_cols] = pick(
            d, every, slice(middle, middle + out_cols)
        )
    for h in range(lanes // sharing):
        for first, out_ref in ((0, k_ref), (1, v_ref)):
            total = None
            for d in range(h * sharing + first, (h + 1) * sharing, 2):
                part = pick(d, every, slice(head_cols, middle))
                total = part if total is None else total + part
            out_ref[:, h * HEAD_DIM : (h + 1) * HEAD_DIM] = total


def spread_down_kernel(lane_ref, mine_ref, other_ref, out_ref):
    core = lane_ref[0] % 2
    mine, other = mine_ref[0].astype(FULL), other_ref[0].astype(FULL)
    out_ref[...] = jnp.where(core == pl.program_id(0) % 2, mine, other)


def spread_call(kernel, lane, mine, other, rows, block, widths):
    chips, _, cols = mine.shape
    spec = pl.BlockSpec((chips, block, cols), lambda i, lane_ref: (0, i, 0))
    return pl.pallas_call(
        kernel,
        out_shape=tuple(jax.ShapeDtypeStruct((rows, w), FULL) for w in widths),
        grid_spec=pltpu.PrefetchScalarGridSpec(
            num_scalar_prefetch=1,
            grid=(rows // block,),
            in_specs=[spec, spec],
            out_specs=tuple(pl.BlockSpec((block, w), lambda i, lane_ref: (i, 0)) for w in widths),
        ),
        cost_estimate=pl.CostEstimate(
            flops=0, bytes_accessed=chips * rows * cols * 12, transcendentals=0
        ),
    )(lane, mine, other)


def spread_down(lane, mine, other):
    chips, rows, cols = mine.shape
    spec = pl.BlockSpec(
        (1, rows, cols), lambda d, lane_ref: ((d // 2) ^ (lane_ref[0] // 2), 0, 0)
    )
    return pl.pallas_call(
        spread_down_kernel,
        out_shape=jax.ShapeDtypeStruct((2 * chips * rows, cols), FULL),
        grid_spec=pltpu.PrefetchScalarGridSpec(
            num_scalar_prefetch=1,
            grid=(2 * chips,),
            in_specs=[spec, spec],
            out_specs=pl.BlockSpec((rows, cols), lambda d, lane_ref: (d, 0)),
        ),
        cost_estimate=pl.CostEstimate(
            flops=0, bytes_accessed=chips * rows * cols * 12, transcendentals=0
        ),
    )(lane, mine, other)


def on_device(
    tokens,
    block_order,
    attn_gain,
    w_query,
    w_key,
    w_value,
    w_out,
    mlp_gain,
    w_gate,
    w_up,
    w_down,
    cotangent,
):
    planes = lax.axis_size(SHARD)
    plane = lax.axis_index(SHARD)
    lanes = lax.axis_size(DP)
    lane = lax.axis_index(DP)
    odd = lax.rem(lane, 2) == 1
    rows = tokens.shape[1]
    width = tokens.shape[2]
    span = rows // 2
    seqs = lanes
    total_rows = seqs * rows
    own_width = width // planes
    heads = w_query.shape[1] // HEAD_DIM
    kv_heads = w_key.shape[1] // HEAD_DIM
    own_heads = heads // lanes
    head_cols = own_heads * HEAD_DIM
    kv_head = (lane * own_heads * kv_heads) // heads
    out_cols = w_out.shape[1] // lanes
    ff_rows = w_down.shape[0]
    unit = ff_rows // lanes
    own_ff = unit * planes
    scale = HEAD_DIM ** (-0.5)

    inputs = lax.all_gather(tokens[0], DP, axis=0, tiled=True)
    upstream = lax.all_gather(cotangent[0], DP, axis=0, tiled=True)
    table = lax.all_gather(block_order[0], DP, axis=0, tiled=False)

    def columns(weight, start, count):
        return lax.dynamic_slice_in_dim(weight, start, count, 1).astype(LOW)

    kv_at = kv_head * HEAD_DIM
    qkv_piece = jnp.concatenate(
        [
            columns(w_query, lane * head_cols, head_cols),
            jnp.where(odd, columns(w_value, kv_at, HEAD_DIM), columns(w_key, kv_at, HEAD_DIM)),
        ],
        axis=1,
    )
    qkv_cols = head_cols + HEAD_DIM
    gain_rows = jnp.stack([attn_gain, mlp_gain]).astype(LOW)
    gain_reps = -(-own_width // qkv_cols)
    gain_rows = jnp.pad(gain_rows, ((0, 0), (0, gain_reps * qkv_cols - own_width)))
    gain_rows = gain_rows.reshape(2 * gain_reps, qkv_cols)
    gain_rows = jnp.pad(gain_rows, ((0, EXTRA - 2 * gain_reps), (0, 0)))
    qkv_parts = plane_parts(jnp.concatenate([qkv_piece, gain_rows], axis=0))
    qkv_mat = assemble(placed([part[:own_width] for part in qkv_parts]))
    gain_parts = [
        part[own_width : own_width + 2 * gain_reps].reshape(2, -1)[:, :own_width]
        for part in qkv_parts
    ]
    gains = assemble(placed(gain_parts), 1)
    gain_one, gain_two = gains[0].astype(FULL), gains[1].astype(FULL)

    mlp_piece = jnp.concatenate(
        [
            columns(weight, p * ff_rows + lane * unit, unit)
            for weight in (w_gate, w_up)
            for p in range(planes)
        ],
        axis=1,
    )
    cut = 128
    first_piece = jnp.concatenate(
        [columns(w_out, lane * out_cols, out_cols), mlp_piece[:, :cut]], axis=1
    )
    second_piece = mlp_piece[:, cut:]
    first_piece, second_piece = lax.optimization_barrier((first_piece, second_piece))
    first_parts = plane_parts(first_piece)
    second_pieces = forwarded(second_piece)
    out_mat = assemble(placed([part[:, :out_cols] for part in first_parts]))
    mlp_mat = jnp.zeros((width, 2 * own_ff), LOW)
    for part, place in placed([part[:, out_cols:] for part in first_parts]):
        mlp_mat = lax.dynamic_update_slice(mlp_mat, part, (place * own_width, 0))
    for part, place in second_pieces[:-1]:
        mlp_mat = lax.dynamic_update_slice(mlp_mat, part, (place * own_width, cut))
    part, place = second_pieces[-1]
    mlp_mat = lax.dynamic_update_slice(mlp_mat, part, (place * own_width, cut))
    down_piece = lax.dynamic_slice_in_dim(w_down, lane * unit, unit, 0).astype(LOW)
    down_mat = assemble(forwarded(down_piece))

    grouped = table.reshape(seqs, planes, 2)
    order = lax.rem(plane - jnp.arange(planes, dtype=jnp.int32) + planes, planes)
    relative = jnp.take(grouped, order, axis=1)
    smaller = jnp.min(relative, axis=2)
    info = jnp.concatenate(
        [
            (relative[:, :, 0] > relative[:, :, 1]).astype(jnp.int32),
            (smaller < smaller[:, :1]).astype(jnp.int32),
        ],
        axis=1,
    )
    places = relative[:, 0, :, None] * span + jnp.arange(span, dtype=jnp.int32)
    frequency = ROPE_BASE ** (-(jnp.arange(HEAD_DIM // 2, dtype=FULL) * 2.0) / HEAD_DIM)
    angles = frequency[:, None] * places.reshape(-1).astype(FULL)[None, :]
    cosine, sine = jnp.cos(angles), jnp.sin(angles)

    wide = inputs.astype(FULL)
    scale_one = lax.rsqrt(jnp.mean(wide * wide, axis=-1, keepdims=True) + EPSILON)
    hidden_one = (wide * scale_one * gain_one).astype(LOW)
    qkv = contract(qkv_mat, hidden_one, 0, 1)
    half = qkv[head_cols:]
    half = jnp.where(odd, half, rope(half, cosine, sine)).astype(LOW)
    half_parts = plane_parts(half)
    query = rope(qkv[:head_cols].reshape(own_heads, HEAD_DIM, total_rows), cosine, sine)
    query = (query.astype(LOW).astype(FULL) * scale).astype(LOW).reshape(head_cols, total_rows)
    half_all = jnp.stack(half_parts, axis=0)
    other_half = swap_cores(half_all)
    key_all = jnp.where(odd, other_half, half_all)
    value_all = jnp.where(odd, half_all, other_half)
    attended, log_total = attn_forward(info, query, key_all, value_all, seqs)

    attended_all = lax.all_gather(attended, DP, axis=0, tiled=True)
    branch = contract(out_mat, attended_all, 0, 0)
    own_inputs = lax.dynamic_slice_in_dim(inputs, lane * out_cols, out_cols, 1)
    out_rows = jnp.zeros((head_cols, lanes * out_cols), LOW)
    for m in range(lanes):
        peer = lane ^ m
        block = lax.dynamic_slice_in_dim(out_mat, peer * head_cols, head_cols, 0)
        if m:
            block = lax.ppermute(block, DP, [(d, d ^ m) for d in range(lanes)])
        out_rows = lax.dynamic_update_slice_in_dim(out_rows, block, peer * out_cols, 1)
    middle_part = (own_inputs.astype(FULL).T + branch).astype(LOW)
    middle = lax.all_gather(middle_part, DP, axis=0, tiled=True)
    wide_two = middle.astype(FULL)
    scale_two = lax.rsqrt(jnp.mean(wide_two * wide_two, axis=0, keepdims=True) + EPSILON)
    hidden_two = (wide_two * scale_two * gain_two[:, None]).astype(LOW)
    both = contract(mlp_mat, hidden_two, 0, 0)
    gate_value, up_value = both[:own_ff], both[own_ff:]
    sigmoid = jax.nn.sigmoid(gate_value)
    silu = gate_value * sigmoid
    inner = (silu * up_value).astype(LOW)

    inner_grad = contract(down_mat, upstream, 1, 1)
    gate_grad = inner_grad * up_value * sigmoid * (1.0 + gate_value * (1.0 - sigmoid))
    up_grad = inner_grad * silu
    both_grad = jnp.concatenate([gate_grad.astype(LOW), up_grad.astype(LOW)], axis=0)
    hidden_two_grad = contract(both_grad, mlp_mat, 0, 1).astype(LOW)
    hidden_two_own = lax.psum_scatter(hidden_two_grad, DP, scatter_dimension=0, tiled=True)
    mlp_grad = contract(hidden_two, both_grad, 1, 1).astype(LOW)
    down_grad = contract(inner, upstream, 1, 0).astype(LOW)
    down_sent = plane_send(down_grad)
    tail = own_width * 3 // 16
    mlp_grad = mlp_grad.reshape(planes, own_width, 2 * own_ff)
    mlp_sent = plane_send(mlp_grad[:, :-tail].reshape(-1, 2 * own_ff))
    mlp_tail_sent = plane_send(mlp_grad[:, -tail:].reshape(-1, 2 * own_ff))
    partial_out = contract(inner, down_mat, 0, 0).astype(LOW)
    hidden_two_own = hidden_two_own.astype(FULL)
    middle_own = lax.dynamic_slice_in_dim(middle, lane * rows, rows, 1).astype(FULL).T
    scale_own = lax.rsqrt(jnp.mean(middle_own * middle_own, axis=-1, keepdims=True) + EPSILON)
    normed_own = middle_own * scale_own
    gain_two_grad = jnp.sum(hidden_two_own * normed_own, axis=0)
    middle_grad = cotangent[0].astype(FULL) + norm_back(
        hidden_two_own, normed_own, scale_own, gain_two
    )
    middle_grad_low = middle_grad.astype(LOW)
    branch_grad = lax.all_gather(middle_grad_low, DP, axis=0, tiled=True)

    partial_out, branch_grad = lax.optimization_barrier((partial_out, branch_grad))
    result = lax.psum_scatter(partial_out, DP, scatter_dimension=0, tiled=True)
    block_out = (middle_own + result.astype(FULL)).astype(LOW)[None]

    attended_grad = contract(out_rows, branch_grad, 1, 1).astype(LOW)
    query_grad, key_grad, value_grad = attn_backward(
        info, query, key_all, value_all, attended, log_total, attended_grad, seqs
    )
    other_grad = swap_cores(jnp.where(odd, key_grad, value_grad))
    half_grad = (
        jnp.where(odd, value_grad, key_grad).astype(FULL) + other_grad.astype(FULL)
    ).astype(LOW)
    half_own = half_grad[0].astype(FULL)
    for k in range(1, planes):
        part = shift(half_grad[k], planes - k)
        half_own = half_own + part.astype(FULL)
    query_lin = rope(query_grad.reshape(own_heads, HEAD_DIM, total_rows), cosine, -sine)
    query_lin = query_lin.astype(LOW).reshape(head_cols, total_rows)
    half_lin = jnp.where(odd, half_own, rope(half_own, cosine, -sine)).astype(LOW)
    qkv_lin = jnp.concatenate([query_lin, half_lin], axis=0)
    hidden_one_part = contract(qkv_lin, qkv_mat, 0, 1)
    hidden_one_low = hidden_one_part.astype(LOW)
    hidden_one_grad = lax.psum_scatter(
        hidden_one_low, DP, scatter_dimension=0, tiled=True
    ).astype(FULL)
    gain_one_grad = jnp.sum(hidden_one_low.astype(FULL) * (wide * scale_one), axis=0)
    own_tokens = tokens[0].astype(FULL)
    own_scale = lax.rsqrt(jnp.mean(own_tokens * own_tokens, axis=-1, keepdims=True) + EPSILON)
    input_norm_grad = norm_back(hidden_one_grad, own_tokens * own_scale, own_scale, gain_one)
    tokens_grad = (middle_grad + input_norm_grad)[None]

    branch_cols = lax.dynamic_slice_in_dim(branch_grad, lane * out_cols, out_cols, 1)
    qkv_grad = contract(hidden_one, qkv_lin, 0, 1).astype(LOW)
    out_grad = contract(attended_all, branch_cols, 1, 0).astype(LOW)
    out_grad = lax.optimization_barrier(out_grad)
    attn_grad = jnp.concatenate([qkv_grad, out_grad], axis=1).reshape(planes, own_width, -1)
    attn_grad = jnp.pad(attn_grad, ((0, 0), (0, 16), (0, 0)))
    attn_sent = plane_send(attn_grad.reshape(planes * (own_width + 16), -1))
    gain_grads = jnp.stack([gain_one_grad, gain_two_grad])
    gain_grads = jnp.transpose(gain_grads.reshape(2, planes, own_width), (1, 0, 2))
    gain_sent = plane_send(gain_grads.reshape(2 * planes, own_width))
    gain_own = sum(gain_sent[1:], gain_sent[0])
    gain_stack = chip_stack(gain_own)
    gain_own = sum(gain_stack[1:], gain_stack[0])
    gain_other = swap_cores(gain_own)
    gain_own = gain_own + gain_other
    gain_one_out, gain_two_out = gain_own[0], gain_own[1]

    down_sum = plane_sum(down_sent)
    down_mine = jnp.stack(chip_stack(down_sum), axis=0)
    down_other = swap_cores(down_mine)
    mlp_sum = plane_sum(mlp_sent)
    mlp_mine = jnp.stack(chip_stack(mlp_sum), axis=0)
    mlp_other = swap_cores(mlp_mine)
    mlp_tail_mine = jnp.stack(chip_stack(plane_sum(mlp_tail_sent)), axis=0)
    mlp_tail_other = swap_cores(mlp_tail_mine)
    mlp_mine = jnp.concatenate([mlp_mine, mlp_tail_mine], axis=1)
    mlp_other = jnp.concatenate([mlp_other, mlp_tail_other], axis=1)
    attn_sum = plane_sum(attn_sent)
    attn_mine = jnp.stack(chip_stack(attn_sum), axis=0)
    attn_other = swap_cores(attn_mine)

    lane_id = lane.astype(jnp.int32).reshape(1)
    if unit % 16 == 0:
        down_out = spread_down(lane_id, down_mine, down_other)
    else:
        down_out = lax.all_gather(down_sum, DP, axis=0, tiled=True).astype(FULL)
    gate_out, up_out = spread_call(
        functools.partial(spread_mlp_kernel, lanes, planes, unit),
        lane_id,
        mlp_mine,
        mlp_other,
        own_width,
        min(64, own_width),
        (lanes * own_ff, lanes * own_ff),
    )
    query_out, key_out, value_out, out_out = spread_call(
        functools.partial(
            spread_attn_kernel, lanes, head_cols, out_cols, lanes // kv_heads
        ),
        lane_id,
        attn_mine,
        attn_other,
        own_width,
        EXTRA,
        (lanes * head_cols, kv_heads * HEAD_DIM, kv_heads * HEAD_DIM, lanes * out_cols),
    )
    return (
        block_out,
        tokens_grad,
        gain_one_out,
        query_out,
        key_out,
        value_out,
        out_out,
        gain_two_out,
        gate_out,
        up_out,
        down_out,
    )


def solution(mesh):
    rows = P(SHARD, None)
    acts = P(DP, SHARD, None)
    gain = P(SHARD)
    weights = (gain, rows, rows, rows, rows, gain, rows, rows, rows)

    return jax.shard_map(
        on_device,
        mesh=mesh,
        in_specs=(acts, P(DP, None)) + weights + (acts,),
        out_specs=(acts, acts) + weights,
        check_vma=False,
    )
```
